256 devices in a mesh: lev: 2 (over core), wa: 128 (over y, z, x).
Axes of the slice: x: 4, y: 4, z: 8, core: 2. Of those that a mesh axis runs over, the one named last changes fastest.
Arguments:
- spectral: bfloat16 [1280, 1280, 2, 64], P('wa', None, None, 'lev'), parts along dimension 3, may hold values from -0.15625 to 0.15625
- legendre: bfloat16 [1280, 1280, 384], P('wa'), may hold values from -0.15625 to 0.15625
- wavenumber: int32 [1280], P('wa'), may hold values from 0 to 1279, each once
Outputs:
- grid: float32 [768, 2560, 64], P('wa', None, 'lev'), parts along dimension 2
The draws below stay inside these ranges and needn't reach their ends.
There are 2 independent parts, one for each index of `lev`. The reference program is written for one: setup_inputs(seed, part) draws one part's arguments, and reference() takes and returns one part's arrays. A program takes and returns all parts, laid end to end along the dimension named above; an argument that names none is the same for every part. Nothing has to cross between parts.
Inputs may be any that keep to these rules, and one draw needn't show every extreme that they name: wavenumber names every number of 0 to 1279 exactly once; slot k of spectral and legendre belongs to wavenumber[k].
All inputs are finite; a program needn't handle non-finite values.
Results may differ from the reference program's by a relative error of at most 0.0003.
Values sent between devices are 32-bit elements.
A program may use at most 128 MiB of HBM per device.

```python
import jax
import jax.numpy as jnp
from jax import lax

TRUNC = 1279
NLON = 2560
LEVELS = 32
WAVES = 1280
NORTH = 384


def level_of(stream_key, dims, shards, low, high):
    def one(axis_at, shards_of):
        heights = jax.random.uniform(jax.random.fold_in(jax.random.fold_in(stream_key, 6), axis_at), (shards_of,), jnp.float32, low / len(shards), high / len(shards))
        return jnp.repeat(jnp.exp(heights), dims[axis_at] // shards_of).reshape((-1,) + (1,) * (len(dims) - axis_at - 1))

    factor_of = one(*shards[0])
    for cut in shards[1:]:
        factor_of = factor_of * one(*cut)
    return factor_of


def scatter_about(rng, shape, deviation, limit, cuts=(), kind=jnp.bfloat16):
    values = deviation * jax.random.normal(rng, shape, jnp.float32)
    if cuts:
        values = values * level_of(rng, shape, cuts, -0.22, 0.18)
    return jnp.clip(values, -limit, limit).astype(kind)


def setup_inputs(seed: int = 0, part: int = 0) -> dict:
    streams_of = jax.random.split(jax.random.key(seed), 4)
    own_keys = jax.random.split(jax.random.fold_in(streams_of[3], part), 4)
    return {
        "spectral": scatter_about(own_keys[0], (WAVES, WAVES, 2, LEVELS), (TRUNC + 1) ** -0.5, 0.15625, ((0, 128),)),
        "legendre": scatter_about(streams_of[1], (WAVES, WAVES, NORTH), (TRUNC + 1) ** -0.5, 0.15625, ((0, 128),)),
        "wavenumber": jax.random.permutation(streams_of[2], TRUNC + 1).astype(jnp.int32),
    }


def reference(spectral, legendre, wavenumber):
    degrees = spectral.shape[1]
    levels = spectral.shape[3]
    row_index = jnp.arange(degrees, dtype=jnp.int32)

    def one_slot(slot_item):
        rows_table, coeffs, slot_wave = slot_item
        coeff_rows = coeffs.reshape(degrees, 2 * levels)
        kept = jnp.where((row_index >= slot_wave)[:, None], coeff_rows, jnp.zeros_like(coeff_rows))
        flipped = jnp.where(((row_index - slot_wave) % 2 == 0)[:, None], kept, -kept)
        north_sums = jnp.dot(rows_table.T, kept, preferred_element_type=jnp.float32)
        south_sums = jnp.dot(rows_table.T, flipped, preferred_element_type=jnp.float32)
        return jnp.concatenate([north_sums, south_sums[::-1]], 0)

    fourier = lax.map(one_slot, (legendre, spectral, wavenumber))
    real_part = fourier[..., :levels]
    imag_part = fourier[..., levels:] * (wavenumber != 0).astype(fourier.dtype)[:, None, None]
    complex_coeffs = lax.complex(real_part, imag_part)
    spectrum = jnp.zeros((NLON // 2 + 1,) + real_part.shape[1:], complex_coeffs.dtype)
    spectrum = spectrum.at[wavenumber].set(complex_coeffs)
    gridded = jnp.fft.irfft(spectrum, n=NLON, axis=0) * NLON
    return jnp.transpose(gridded, (1, 0, 2)).astype(jnp.float32)
```

```python
import functools
import math

import jax
import jax.numpy as jnp
from jax import lax
from jax.experimental import pallas as pl
from jax.experimental.pallas import tpu as pltpu
from jax.sharding import PartitionSpec as P

NLON = 2560
TILE = 256
LANES = 128
NY, NZ, NX = 4, 8, 4
PLANE = NY * NX
OWNERS = NY * NZ * NX


def cos_sin(turns):
    quarter = jnp.floor(turns * (4.0 / NLON) + 0.5)
    x = (turns - quarter * (NLON // 4)) * (2.0 * math.pi / NLON)
    y = x * x
    s = x * (1.0 + y * (-1 / 6 + y * (1 / 120 + y * (-1 / 5040 + y * (1 / 362880)))))
    c = 1.0 + y * (-1 / 2 + y * (1 / 24 + y * (-1 / 720 + y * (1 / 40320 - y * (1 / 3628800)))))
    which = quarter.astype(jnp.int32) & 3
    odd = (which & 1) == 1
    cos_out = jnp.where(odd, s, c)
    sin_out = jnp.where(odd, c, s)
    cos_out = jnp.where((which == 1) | (which == 2), -cos_out, cos_out)
    sin_out = jnp.where(which >= 2, -sin_out, sin_out)
    return cos_out, sin_out


def transform_kernel(
    chunks, rows,
    wave_smem, spectral_hbm, legendre_hbm,
    out,
    spectral, legendre, staged, send, middle, recv,
    wave_row, wave_mid, wave_all, wave_rows,
    cos_hi, cos_lo, sin_hi, sin_lo, even, odd,
    load_sem, z_send, z_recv, p_send, p_recv, own_sem,
):
    me = lax.axis_index("wa")
    y, z, x = me // (NZ * NX), (me // NX) % NZ, me % NX
    place = y * NX + x
    slots, columns, degrees = spectral.shape
    north = legendre.shape[2]
    levels = columns // 2

    def peer_at(py, pz, px):
        return (py * NZ + pz) * NX + px

    def remote(src, dst, send_sem, recv_sem, peer):
        return pltpu.make_async_remote_copy(
            src_ref=src, dst_ref=dst, send_sem=send_sem, recv_sem=recv_sem,
            device_id={"wa": peer}, device_id_type=pl.DeviceIdType.MESH,
        )

    def each_z(act):
        for d in (4, 3, 5, 2, 6, 1, 7):
            act((z + d) % NZ)

    def each_place(act):
        for d in (5, 10, 15, 2, 8, 7, 13, 1, 4, 3, 12, 6, 9, 11, 14):
            act((y + d // NX) % NY, (x + d % NX) % NX)

    def z_copy(c, to, owner):
        return remote(
            send.at[c, :, to, :, 0:rows, :], middle.at[c, owner, :, :, 0:rows, :],
            z_send.at[c, to], z_recv.at[c, owner], peer_at(y, to, x),
        )

    def z_own(c):
        return pltpu.make_async_copy(
            send.at[c, :, z, :, 0:rows, :], middle.at[c, z, :, :, 0:rows, :], own_sem.at[0, c]
        )

    def p_copy(c, py, px, owner):
        return remote(
            middle.at[c, :, py, px, 0:rows, :], recv.at[c, owner, :, 0:rows, :],
            p_send.at[c, py * NX + px], p_recv.at[c, owner], peer_at(py, z, px),
        )

    def p_own(c):
        return pltpu.make_async_copy(
            middle.at[c, :, y, x, 0:rows, :], recv.at[c, place, :, 0:rows, :], own_sem.at[1, c]
        )

    def wave_z(to, owner):
        return remote(
            wave_row.at[0:1, :], wave_mid.at[owner, 0:1, :],
            z_send.at[chunks, to], z_recv.at[chunks, owner], peer_at(y, to, x),
        )

    wave_z_own = pltpu.make_async_copy(
        wave_row.at[0:1, :], wave_mid.at[z, 0:1, :], own_sem.at[0, chunks]
    )

    def wave_p(py, px, owner):
        return remote(
            wave_mid.at[:, 0:1, :], wave_all.at[owner, :, 0:1, :],
            p_send.at[chunks, py * NX + px], p_recv.at[chunks, owner], peer_at(py, z, px),
        )

    wave_p_own = pltpu.make_async_copy(
        wave_mid.at[:, 0:1, :], wave_all.at[place, :, 0:1, :], own_sem.at[1, chunks]
    )

    def load(slot):
        return (
            pltpu.make_async_copy(spectral_hbm.at[slot], spectral.at[slot], load_sem.at[0, slot]),
            pltpu.make_async_copy(legendre_hbm.at[slot], legendre.at[slot], load_sem.at[1, slot]),
        )

    for slot in range(slots):
        for copy in load(slot):
            copy.start()

    barrier = pltpu.get_barrier_semaphore()

    def greet(peer):
        pl.semaphore_signal(
            barrier, inc=1, device_id={"wa": peer}, device_id_type=pl.DeviceIdType.MESH
        )

    each_z(lambda to: greet(peer_at(y, to, x)))
    each_place(lambda py, px: greet(peer_at(py, z, px)))
    at_slot = lax.broadcasted_iota(jnp.int32, wave_row.shape, 1)
    waves = jnp.zeros(wave_row.shape, jnp.int32)
    for slot in range(slots):
        waves = jnp.where(at_slot == slot, wave_smem[slot], waves)
    wave_row[...] = waves
    staged[...] = jnp.zeros(staged.shape, jnp.float32)
    pl.semaphore_wait(barrier, NZ - 1 + PLANE - 1)
    each_z(lambda to: wave_z(to, z).start())
    wave_z_own.start()

    index = lax.broadcasted_iota(jnp.int32, (1, degrees), 1)

    def sums_of(slot):
        for copy in load(slot):
            copy.wait()
        offset = index - wave_smem[slot]
        keep = jnp.where(offset >= 0, 1.0, 0.0)
        flip = jnp.where((offset & 1) == 0, keep, -keep)
        coeff = spectral[slot]
        both = jnp.concatenate(
            [coeff * keep.astype(coeff.dtype), coeff * flip.astype(coeff.dtype)], 0
        )
        return jnp.dot(both, legendre[slot], preferred_element_type=jnp.float32)

    def synthesize(c, carry):
        first = sums_of(2 * c)
        second = sums_of(2 * c + 1)
        for side in range(2):
            part = slice(side * columns, (side + 1) * columns)
            staged[side, 0:north, :] = jnp.concatenate([first[part], second[part]], 0).T
            for slab in range(OWNERS // 2):
                d = OWNERS - 1 - slab if side else slab
                send[c, d // (NZ * NX), (d // NX) % NZ, d % NX] = staged[
                    side, rows * slab:rows * slab + 8, :
                ]
        each_z(lambda to: z_copy(c, to, z).start())
        z_own(c).start()
        return carry

    lax.fori_loop(0, chunks, synthesize, 0)

    wave_z_own.wait()
    each_z(lambda to: wave_z(to, to).wait_recv())
    each_place(lambda py, px: wave_p(py, px, place).start())
    wave_p_own.start()
    even[...] = jnp.zeros(even.shape, jnp.float32)
    odd[...] = jnp.zeros(odd.shape, jnp.float32)

    wave_p_own.wait()
    each_place(lambda py, px: wave_p(py, px, py * NX + px).wait_recv())
    flat_waves = wave_all.reshape(OWNERS * 8, LANES)
    gathered = flat_waves[pl.ds(0, OWNERS, stride=8), :].astype(jnp.float32)
    for slot in range(slots):
        wave_rows[slot * OWNERS:(slot + 1) * OWNERS, :] = jnp.broadcast_to(
            gathered[:, slot:slot + 1], (OWNERS, LANES)
        )
    position = lax.broadcasted_iota(jnp.int32, (1, LANES), 1).astype(jnp.float32)
    sin_tiles = sin_hi.shape[1] // LANES

    def fill(i, carry):
        at = pl.ds(pl.multiple_of(i * 16, 16), 16)
        waves = wave_rows[at, :]
        weight = jnp.where(waves == 0.0, 1.0, 2.0)
        c, s = cos_sin(waves * position)
        turn_c, turn_s = cos_sin(waves * float(LANES))
        c, s = c * weight, s * weight
        for tile in range(sin_tiles + 1):
            to = slice(tile * LANES, (tile + 1) * LANES)
            top = c.astype(jnp.bfloat16)
            cos_hi[at, to] = top
            cos_lo[at, to] = (c - top.astype(jnp.float32)).astype(jnp.bfloat16)
            if tile < sin_tiles:
                top = s.astype(jnp.bfloat16)
                sin_hi[at, to] = top
                sin_lo[at, to] = (s - top.astype(jnp.float32)).astype(jnp.bfloat16)
                c, s = c * turn_c - s * turn_s, s * turn_c + c * turn_s
        return carry

    south = me // (OWNERS // 2)
    flat = recv.reshape(chunks * OWNERS * 8, LANES)

    def forward(c):
        z_own(c).wait()
        each_z(lambda to: z_copy(c, to, to).wait_recv())
        each_place(lambda py, px: p_copy(c, py, px, place).start())
        p_own(c).start()

    def add_chunk(c):
        p_own(c).wait()
        each_place(lambda py, px: p_copy(c, py, px, py * NX + px).wait_recv())
        parts = [[], []]
        for row in range(rows):
            source = row + south * (rows - 1 - 2 * row)
            turned = flat[pl.ds(c * OWNERS * 8 + source, OWNERS, stride=8), :].T
            for part in range(2):
                parts[part].append(
                    jnp.concatenate(
                        [turned[part * levels:(part + 1) * levels],
                         turned[(2 + part) * levels:(3 + part) * levels]], 1
                    )
                )
        at = pl.ds(pl.multiple_of(c * 2 * OWNERS, 2 * OWNERS), 2 * OWNERS)
        for part, total, high, low in ((0, even, cos_hi, cos_lo), (1, odd, sin_hi, sin_lo)):
            values = jnp.concatenate(parts[part], 0)
            top = values.astype(jnp.bfloat16)
            rest = (values - top.astype(jnp.float32)).astype(jnp.bfloat16)
            table = high[at, :]
            sums = jnp.dot(top, table, preferred_element_type=jnp.float32)
            sums += jnp.dot(rest, table, preferred_element_type=jnp.float32)
            sums += jnp.dot(top, low[at, :], preferred_element_type=jnp.float32)
            total[...] += sums

    forward(0)
    lax.fori_loop(0, wave_rows.shape[0] // 16, fill, 0)

    def later(c, carry):
        @pl.when(c < chunks)
        def _():
            forward(c)

        add_chunk(c - 1)
        return carry

    lax.fori_loop(1, chunks + 1, later, 0)

    r = lax.broadcasted_iota(jnp.int32, (TILE, TILE), 0)
    q = lax.broadcasted_iota(jnp.int32, (TILE, TILE), 1)
    mirror = jnp.where(r + q == TILE, 1.0, 0.0).astype(jnp.bfloat16)
    at_zero = lax.broadcasted_iota(jnp.int32, (1, TILE), 1) == 0
    tiles = odd.shape[1] // TILE
    after = even[:, tiles * TILE:tiles * TILE + 1]
    for tile in range(tiles - 1, -1, -1):
        to = slice(tile * TILE, (tile + 1) * TILE)
        back = slice((2 * tiles - 1 - tile) * TILE, (2 * tiles - tile) * TILE)
        e, o = even[:, to], odd[:, to]
        out[:, :, to] = (e - o).reshape(rows, levels, TILE)
        d = e + o
        top = d.astype(jnp.bfloat16)
        rest = (d - top.astype(jnp.float32)).astype(jnp.bfloat16)
        turned = jnp.dot(top, mirror, preferred_element_type=jnp.float32)
        turned += jnp.dot(rest, mirror, preferred_element_type=jnp.float32)
        out[:, :, back] = jnp.where(at_zero, after, turned).reshape(rows, levels, TILE)
        after = d[:, 0:1]

    each_z(lambda to: wave_z(to, z).wait_send())
    each_place(lambda py, px: wave_p(py, px, place).wait_send())

    def drain(c, carry):
        each_z(lambda to: z_copy(c, to, z).wait_send())
        each_place(lambda py, px: p_copy(c, py, px, place).wait_send())
        return carry

    lax.fori_loop(0, chunks, drain, 0)


def on_device(spectral, legendre, wavenumber):
    slots, degrees, _, levels = spectral.shape
    north = legendre.shape[2]
    rows = 2 * north // OWNERS
    chunks = slots // 2
    coeff = jnp.transpose(spectral, (0, 2, 3, 1)).reshape(slots, 2 * levels, degrees)
    depth = slots * OWNERS
    half = NLON // 2
    f32, bf16, i32 = jnp.float32, jnp.bfloat16, jnp.int32
    grid = pl.pallas_call(
        functools.partial(transform_kernel, chunks, rows),
        out_shape=jax.ShapeDtypeStruct((rows, levels, NLON), f32),
        in_specs=[
            pl.BlockSpec(memory_space=pltpu.SMEM),
            pl.BlockSpec(memory_space=pltpu.HBM),
            pl.BlockSpec(memory_space=pltpu.HBM),
        ],
        out_specs=pl.BlockSpec(memory_space=pltpu.VMEM),
        scratch_shapes=[
            pltpu.VMEM((slots, 2 * levels, degrees), bf16),
            pltpu.VMEM((slots, degrees, north), bf16),
            pltpu.VMEM((2, north + 8, LANES), f32),
            pltpu.VMEM((chunks, NY, NZ, NX, 8, LANES), f32),
            pltpu.VMEM((chunks, NZ, NY, NX, 8, LANES), f32),
            pltpu.VMEM((chunks, PLANE, NZ, 8, LANES), f32),
            pltpu.VMEM((8, LANES), i32),
            pltpu.VMEM((NZ, 8, LANES), i32),
            pltpu.VMEM((PLANE, NZ, 8, LANES), i32),
            pltpu.VMEM((depth, LANES), f32),
            pltpu.VMEM((depth, half + LANES), bf16),
            pltpu.VMEM((depth, half + LANES), bf16),
            pltpu.VMEM((depth, half), bf16),
            pltpu.VMEM((depth, half), bf16),
            pltpu.VMEM((rows * levels, half + LANES), f32),
            pltpu.VMEM((rows * levels, half), f32),
            pltpu.SemaphoreType.DMA((2, slots)),
            pltpu.SemaphoreType.DMA((chunks + 1, NZ)),
            pltpu.SemaphoreType.DMA((chunks + 1, NZ)),
            pltpu.SemaphoreType.DMA((chunks + 1, PLANE)),
            pltpu.SemaphoreType.DMA((chunks + 1, PLANE)),
            pltpu.SemaphoreType.DMA((2, chunks + 1)),
        ],
        compiler_params=pltpu.CompilerParams(
            collective_id=0, has_side_effects=True, vmem_limit_bytes=60 * 2**20,
        ),
    )(wavenumber, coeff, legendre)
    return jnp.transpose(grid, (0, 2, 1))


def solution(mesh):
    return jax.shard_map(
        on_device,
        mesh=mesh,
        in_specs=(P("wa", None, None, "lev"), P("wa", None, None), P("wa")),
        out_specs=P("wa", None, "lev"),
        check_vma=False,
    )
```

```python
import functools
import math

import jax
import jax.numpy as jnp
from jax import lax
from jax.experimental import pallas as pl
from jax.experimental.pallas import tpu as pltpu
from jax.sharding import PartitionSpec as P

NLON = 2560
TILE = 256
LANES = 128
NY, NZ, NX = 4, 8, 4
PLANE = NY * NX
OWNERS = NY * NZ * NX


def cos_sin(turns):
    quarter = jnp.floor(turns * (4.0 / NLON) + 0.5)
    x = (turns - quarter * (NLON // 4)) * (2.0 * math.pi / NLON)
    y = x * x
    s = x * (1.0 + y * (-1 / 6 + y * (1 / 120 + y * (-1 / 5040 + y * (1 / 362880)))))
    c = 1.0 + y * (-1 / 2 + y * (1 / 24 + y * (-1 / 720 + y * (1 / 40320 - y * (1 / 3628800)))))
    which = quarter.astype(jnp.int32) & 3
    odd = (which & 1) == 1
    cos_out = jnp.where(odd, s, c)
    sin_out = jnp.where(odd, c, s)
    cos_out = jnp.where((which == 1) | (which == 2), -cos_out, cos_out)
    sin_out = jnp.where(which >= 2, -sin_out, sin_out)
    return cos_out, sin_out


def transform_kernel(
    chunks, line_first, rows,
    wave_smem, spectral_hbm, legendre_hbm,
    out,
    spectral, legendre, staged, send, middle, spread, recv,
    wave_row, wave_mid, wave_all, wave_rows,
    cos_hi, cos_lo, sin_hi, sin_lo, even, odd,
    load_sem, z_send, z_recv, p_send, p_recv, own_sem,
):
    me = lax.axis_index("wa")
    y, z, x = me // (NZ * NX), (me // NX) % NZ, me % NX
    place = y * NX + x
    slots, columns, degrees = spectral.shape
    north = legendre.shape[2]
    levels = columns // 2

    def peer_at(py, pz, px):
        return (py * NZ + pz) * NX + px

    def remote(src, dst, send_sem, recv_sem, peer):
        return pltpu.make_async_remote_copy(
            src_ref=src, dst_ref=dst, send_sem=send_sem, recv_sem=recv_sem,
            device_id={"wa": peer}, device_id_type=pl.DeviceIdType.MESH,
        )

    def each_z(act):
        for d in (4, 3, 5, 2, 6, 1, 7):
            act((z + d) % NZ)

    def each_place(act):
        for d in (5, 15, 7, 13, 10, 6, 9, 14, 11, 2, 8, 1, 4, 3, 12):
            act((y + d // NX) % NY, (x + d % NX) % NX)

    def z_copy(c, to, owner):
        if c < line_first:
            src, dst = send.at[c, :, to, :, 0:rows, :], middle.at[c, owner, :, :, 0:rows, :]
        else:
            src = spread.at[c - line_first, :, to, 0:rows, :]
            dst = recv.at[c, :, owner, 0:rows, :]
        return remote(src, dst, z_send.at[c, to], z_recv.at[c, owner], peer_at(y, to, x))

    def z_own(c):
        if c < line_first:
            src, dst = send.at[c, :, z, :, 0:rows, :], middle.at[c, z, :, :, 0:rows, :]
        else:
            src = spread.at[c - line_first, :, z, 0:rows, :]
            dst = recv.at[c, :, z, 0:rows, :]
        return pltpu.make_async_copy(src, dst, own_sem.at[0, c])

    def p_copy(c, py, px, owner):
        if c < line_first:
            src, dst = middle.at[c, :, py, px, 0:rows, :], recv.at[c, owner, :, 0:rows, :]
        else:
            src = send.at[c, py, :, px, 0:rows, :]
            dst = spread.at[c - line_first, owner, :, 0:rows, :]
        return remote(
            src, dst, p_send.at[c, py * NX + px], p_recv.at[c, owner], peer_at(py, z, px)
        )

    def p_own(c):
        if c < line_first:
            src, dst = middle.at[c, :, y, x, 0:rows, :], recv.at[c, place, :, 0:rows, :]
        else:
            src = send.at[c, y, :, x, 0:rows, :]
            dst = spread.at[c - line_first, place, :, 0:rows, :]
        return pltpu.make_async_copy(src, dst, own_sem.at[1, c])

    def start_z(c):
        each_z(lambda to: z_copy(c, to, z).start())
        z_own(c).start()

    def start_p(c):
        each_place(lambda py, px: p_copy(c, py, px, place).start())
        p_own(c).start()

    def wait_z(c):
        z_own(c).wait()
        each_z(lambda to: z_copy(c, to, to).wait_recv())

    def wait_p(c):
        p_own(c).wait()
        each_place(lambda py, px: p_copy(c, py, px, py * NX + px).wait_recv())

    def wave_z(to, owner):
        return remote(
            wave_row.at[0:1, :], wave_mid.at[owner, 0:1, :],
            z_send.at[chunks, to], z_recv.at[chunks, owner], peer_at(y, to, x),
        )

    wave_z_own = pltpu.make_async_copy(
        wave_row.at[0:1, :], wave_mid.at[z, 0:1, :], own_sem.at[0, chunks]
    )

    def wave_p(py, px, owner):
        return remote(
            wave_mid.at[:, 0:1, :], wave_all.at[owner, :, 0:1, :],
            p_send.at[chunks, py * NX + px], p_recv.at[chunks, owner], peer_at(py, z, px),
        )

    wave_p_own = pltpu.make_async_copy(
        wave_mid.at[:, 0:1, :], wave_all.at[place, :, 0:1, :], own_sem.at[1, chunks]
    )

    def load(slot):
        return (
            pltpu.make_async_copy(spectral_hbm.at[slot], spectral.at[slot], load_sem.at[0, slot]),
            pltpu.make_async_copy(legendre_hbm.at[slot], legendre.at[slot], load_sem.at[1, slot]),
        )

    for slot in range(slots):
        for copy in load(slot):
            copy.start()

    barrier = pltpu.get_barrier_semaphore()

    def greet(peer):
        pl.semaphore_signal(
            barrier, inc=1, device_id={"wa": peer}, device_id_type=pl.DeviceIdType.MESH
        )

    each_z(lambda to: greet(peer_at(y, to, x)))
    each_place(lambda py, px: greet(peer_at(py, z, px)))
    at_slot = lax.broadcasted_iota(jnp.int32, wave_row.shape, 1)
    waves = jnp.zeros(wave_row.shape, jnp.int32)
    for slot in range(slots):
        waves = jnp.where(at_slot == slot, wave_smem[slot], waves)
    wave_row[...] = waves
    staged[...] = jnp.zeros(staged.shape, jnp.float32)
    pl.semaphore_wait(barrier, NZ - 1 + PLANE - 1)
    each_z(lambda to: wave_z(to, z).start())
    wave_z_own.start()

    first_order = (0, 3, 1, 4, 2)
    index = lax.broadcasted_iota(jnp.int32, (1, degrees), 1)

    def sums_of(slot):
        for copy in load(slot):
            copy.wait()
        offset = index - wave_smem[slot]
        keep = jnp.where(offset >= 0, 1.0, 0.0)
        flip = jnp.where((offset & 1) == 0, keep, -keep)
        coeff = spectral[slot]
        both = jnp.concatenate(
            [coeff * keep.astype(coeff.dtype), coeff * flip.astype(coeff.dtype)], 0
        )
        return jnp.dot(both, legendre[slot], preferred_element_type=jnp.float32)

    def synthesize(c):
        first = sums_of(2 * c)
        second = sums_of(2 * c + 1)
        for side in range(2):
            part = slice(side * columns, (side + 1) * columns)
            staged[side, 0:north, :] = jnp.concatenate([first[part], second[part]], 0).T
            for slab in range(OWNERS // 2):
                d = OWNERS - 1 - slab if side else slab
                send[c, d // (NZ * NX), (d // NX) % NZ, d % NX] = staged[
                    side, rows * slab:rows * slab + 8, :
                ]

    for c in first_order:
        synthesize(c)
        if c < line_first:
            start_z(c)
        else:
            start_p(c)

    wave_z_own.wait()
    each_z(lambda to: wave_z(to, to).wait_recv())
    each_place(lambda py, px: wave_p(py, px, place).start())
    wave_p_own.start()
    even[...] = jnp.zeros(even.shape, jnp.float32)
    odd[...] = jnp.zeros(odd.shape, jnp.float32)

    wave_p_own.wait()
    each_place(lambda py, px: wave_p(py, px, py * NX + px).wait_recv())
    flat_waves = wave_all.reshape(OWNERS * 8, LANES)
    gathered = flat_waves[pl.ds(0, OWNERS, stride=8), :].astype(jnp.float32)
    for slot in range(slots):
        wave_rows[slot * OWNERS:(slot + 1) * OWNERS, :] = jnp.broadcast_to(
            gathered[:, slot:slot + 1], (OWNERS, LANES)
        )
    position = lax.broadcasted_iota(jnp.int32, (1, LANES), 1).astype(jnp.float32)
    sin_tiles = sin_hi.shape[1] // LANES

    def fill(i, carry):
        at = pl.ds(pl.multiple_of(i * 16, 16), 16)
        waves = wave_rows[at, :]
        weight = jnp.where(waves == 0.0, 1.0, 2.0)
        c, s = cos_sin(waves * position)
        turn_c, turn_s = cos_sin(waves * float(LANES))
        c, s = c * weight, s * weight
        for tile in range(sin_tiles + 1):
            to = slice(tile * LANES, (tile + 1) * LANES)
            top = c.astype(jnp.bfloat16)
            cos_hi[at, to] = top
            cos_lo[at, to] = (c - top.astype(jnp.float32)).astype(jnp.bfloat16)
            if tile < sin_tiles:
                top = s.astype(jnp.bfloat16)
                sin_hi[at, to] = top
                sin_lo[at, to] = (s - top.astype(jnp.float32)).astype(jnp.bfloat16)
                c, s = c * turn_c - s * turn_s, s * turn_c + c * turn_s
        return carry

    south = me // (OWNERS // 2)
    flat = recv.reshape(chunks * OWNERS * 8, LANES)

    def add_chunk(c):
        parts = [[], []]
        for row in range(rows):
            source = row + south * (rows - 1 - 2 * row)
            turned = flat[pl.ds(c * OWNERS * 8 + source, OWNERS, stride=8), :].T
            for part in range(2):
                parts[part].append(
                    jnp.concatenate(
                        [turned[part * levels:(part + 1) * levels],
                         turned[(2 + part) * levels:(3 + part) * levels]], 1
                    )
                )
        at = pl.ds(pl.multiple_of(c * 2 * OWNERS, 2 * OWNERS), 2 * OWNERS)
        for part, total, high, low in ((0, even, cos_hi, cos_lo), (1, odd, sin_hi, sin_lo)):
            values = jnp.concatenate(parts[part], 0)
            top = values.astype(jnp.bfloat16)
            rest = (values - top.astype(jnp.float32)).astype(jnp.bfloat16)
            table = high[at, :]
            sums = jnp.dot(top, table, preferred_element_type=jnp.float32)
            sums += jnp.dot(rest, table, preferred_element_type=jnp.float32)
            sums += jnp.dot(top, low[at, :], preferred_element_type=jnp.float32)
            total[...] += sums

    wait_z(0)
    start_p(0)
    lax.fori_loop(0, wave_rows.shape[0] // 16, fill, 0)
    for c in range(1, line_first):
        wait_z(c)
        start_p(c)
        if line_first - 1 + c < chunks:
            wait_p(line_first - 1 + c)
            start_z(line_first - 1 + c)
        wait_p(c - 1)
        add_chunk(c - 1)
    wait_p(line_first - 1)
    add_chunk(line_first - 1)
    for c in range(line_first, chunks):
        wait_z(c)
        add_chunk(c)

    r = lax.broadcasted_iota(jnp.int32, (TILE, TILE), 0)
    q = lax.broadcasted_iota(jnp.int32, (TILE, TILE), 1)
    mirror = jnp.where(r + q == TILE, 1.0, 0.0).astype(jnp.bfloat16)
    at_zero = lax.broadcasted_iota(jnp.int32, (1, TILE), 1) == 0
    tiles = odd.shape[1] // TILE
    after = even[:, tiles * TILE:tiles * TILE + 1]
    for tile in range(tiles - 1, -1, -1):
        to = slice(tile * TILE, (tile + 1) * TILE)
        back = slice((2 * tiles - 1 - tile) * TILE, (2 * tiles - tile) * TILE)
        e, o = even[:, to], odd[:, to]
        out[:, :, to] = (e - o).reshape(rows, levels, TILE)
        d = e + o
        top = d.astype(jnp.bfloat16)
        rest = (d - top.astype(jnp.float32)).astype(jnp.bfloat16)
        turned = jnp.dot(top, mirror, preferred_element_type=jnp.float32)
        turned += jnp.dot(rest, mirror, preferred_element_type=jnp.float32)
        out[:, :, back] = jnp.where(at_zero, after, turned).reshape(rows, levels, TILE)
        after = d[:, 0:1]

    each_z(lambda to: wave_z(to, z).wait_send())
    each_place(lambda py, px: wave_p(py, px, place).wait_send())

    for c in range(chunks):
        each_z(lambda to: z_copy(c, to, z).wait_send())
        each_place(lambda py, px: p_copy(c, py, px, place).wait_send())


def on_device(spectral, legendre, wavenumber):
    slots, degrees, _, levels = spectral.shape
    north = legendre.shape[2]
    rows = 2 * north // OWNERS
    chunks = slots // 2
    line_first = 3
    coeff = jnp.transpose(spectral, (0, 2, 3, 1)).reshape(slots, 2 * levels, degrees)
    depth = slots * OWNERS
    half = NLON // 2
    f32, bf16, i32 = jnp.float32, jnp.bfloat16, jnp.int32
    grid = pl.pallas_call(
        functools.partial(transform_kernel, chunks, line_first, rows),
        out_shape=jax.ShapeDtypeStruct((rows, levels, NLON), f32),
        in_specs=[
            pl.BlockSpec(memory_space=pltpu.SMEM),
            pl.BlockSpec(memory_space=pltpu.HBM),
            pl.BlockSpec(memory_space=pltpu.HBM),
        ],
        out_specs=pl.BlockSpec(memory_space=pltpu.VMEM),
        scratch_shapes=[
            pltpu.VMEM((slots, 2 * levels, degrees), bf16),
            pltpu.VMEM((slots, degrees, north), bf16),
            pltpu.VMEM((2, north + 8, LANES), f32),
            pltpu.VMEM((chunks, NY, NZ, NX, 8, LANES), f32),
            pltpu.VMEM((line_first, NZ, NY, NX, 8, LANES), f32),
            pltpu.VMEM((chunks - line_first, PLANE, NZ, 8, LANES), f32),
            pltpu.VMEM((chunks, PLANE, NZ, 8, LANES), f32),
            pltpu.VMEM((8, LANES), i32),
            pltpu.VMEM((NZ, 8, LANES), i32),
            pltpu.VMEM((PLANE, NZ, 8, LANES), i32),
            pltpu.VMEM((depth, LANES), f32),
            pltpu.VMEM((depth, half + LANES), bf16),
            pltpu.VMEM((depth, half + LANES), bf16),
            pltpu.VMEM((depth, half), bf16),
            pltpu.VMEM((depth, half), bf16),
            pltpu.VMEM((rows * levels, half + LANES), f32),
            pltpu.VMEM((rows * levels, half), f32),
            pltpu.SemaphoreType.DMA((2, slots)),
            pltpu.SemaphoreType.DMA((chunks + 1, NZ)),
            pltpu.SemaphoreType.DMA((chunks + 1, NZ)),
            pltpu.SemaphoreType.DMA((chunks + 1, PLANE)),
            pltpu.SemaphoreType.DMA((chunks + 1, PLANE)),
            pltpu.SemaphoreType.DMA((2, chunks + 1)),
        ],
        compiler_params=pltpu.CompilerParams(
            collective_id=0, has_side_effects=True, vmem_limit_bytes=60 * 2**20,
        ),
    )(wavenumber, coeff, legendre)
    return jnp.transpose(grid, (0, 2, 1))


def solution(mesh):
    return jax.shard_map(
        on_device,
        mesh=mesh,
        in_specs=(P("wa", None, None, "lev"), P("wa", None, None), P("wa")),
        out_specs=P("wa", None, "lev"),
        check_vma=False,
    )
```

```python
import functools
import math

import jax
import jax.numpy as jnp
from jax import lax
from jax.experimental import pallas as pl
from jax.experimental.pallas import tpu as pltpu
from jax.sharding import PartitionSpec as P

NLON = 2560
TILE = 256
LANES = 128
NY, NZ, NX = 4, 8, 4
PLANE = NY * NX
OWNERS = NY * NZ * NX


def cos_sin(turns):
    quarter = jnp.floor(turns * (4.0 / NLON) + 0.5)
    x = (turns - quarter * (NLON // 4)) * (2.0 * math.pi / NLON)
    y = x * x
    s = x * (1.0 + y * (-1 / 6 + y * (1 / 120 + y * (-1 / 5040 + y * (1 / 362880)))))
    c = 1.0 + y * (-1 / 2 + y * (1 / 24 + y * (-1 / 720 + y * (1 / 40320 - y * (1 / 3628800)))))
    which = quarter.astype(jnp.int32) & 3
    odd = (which & 1) == 1
    cos_out = jnp.where(odd, s, c)
    sin_out = jnp.where(odd, c, s)
    cos_out = jnp.where((which == 1) | (which == 2), -cos_out, cos_out)
    sin_out = jnp.where(which >= 2, -sin_out, sin_out)
    return cos_out, sin_out


def transform_kernel(
    chunks, line_first, rows,
    wave_smem, spectral_hbm, legendre_hbm,
    out,
    spectral, legendre, staged, send, middle, spread, recv,
    wave_row, wave_mid, wave_all, wave_rows,
    cos_hi, cos_lo, sin_hi, sin_lo, even, odd,
    load_sem, z_send, z_recv, p_send, p_recv, own_sem,
):
    me = lax.axis_index("wa")
    y, z, x = me // (NZ * NX), (me // NX) % NZ, me % NX
    place = y * NX + x
    slots, columns, degrees = spectral.shape
    north = legendre.shape[2]
    levels = columns // 2

    def peer_at(py, pz, px):
        return (py * NZ + pz) * NX + px

    def remote(src, dst, send_sem, recv_sem, peer):
        return pltpu.make_async_remote_copy(
            src_ref=src, dst_ref=dst, send_sem=send_sem, recv_sem=recv_sem,
            device_id={"wa": peer}, device_id_type=pl.DeviceIdType.MESH,
        )

    def each_z(act):
        for d in (4, 3, 5, 2, 6, 1, 7):
            act((z + d) % NZ)

    def each_place(act):
        for d in (5, 15, 7, 13, 10, 6, 9, 14, 11, 2, 8, 1, 4, 3, 12):
            act((y + d // NX) % NY, (x + d % NX) % NX)

    def z_copy(c, to, owner):
        if c < line_first:
            src, dst = send.at[c, :, to, :, 0:rows, :], middle.at[c, owner, :, :, 0:rows, :]
        else:
            src = spread.at[c - line_first, :, to, 0:rows, :]
            dst = recv.at[c, :, owner, 0:rows, :]
        return remote(src, dst, z_send.at[c, to], z_recv.at[c, owner], peer_at(y, to, x))

    def z_own(c):
        if c < line_first:
            src, dst = send.at[c, :, z, :, 0:rows, :], middle.at[c, z, :, :, 0:rows, :]
        else:
            src = spread.at[c - line_first, :, z, 0:rows, :]
            dst = recv.at[c, :, z, 0:rows, :]
        return pltpu.make_async_copy(src, dst, own_sem.at[0, c])

    def p_copy(c, py, px, owner):
        if c < line_first:
            src, dst = middle.at[c, :, py, px, 0:rows, :], recv.at[c, owner, :, 0:rows, :]
        else:
            src = send.at[c, py, :, px, 0:rows, :]
            dst = spread.at[c - line_first, owner, :, 0:rows, :]
        return remote(
            src, dst, p_send.at[c, py * NX + px], p_recv.at[c, owner], peer_at(py, z, px)
        )

    def p_own(c):
        if c < line_first:
            src, dst = middle.at[c, :, y, x, 0:rows, :], recv.at[c, place, :, 0:rows, :]
        else:
            src = send.at[c, y, :, x, 0:rows, :]
            dst = spread.at[c - line_first, place, :, 0:rows, :]
        return pltpu.make_async_copy(src, dst, own_sem.at[1, c])

    def start_z(c):
        each_z(lambda to: z_copy(c, to, z).start())
        z_own(c).start()

    def start_p(c):
        each_place(lambda py, px: p_copy(c, py, px, place).start())
        p_own(c).start()

    def wait_z(c):
        z_own(c).wait()
        each_z(lambda to: z_copy(c, to, to).wait_recv())

    def wait_p(c):
        p_own(c).wait()
        each_place(lambda py, px: p_copy(c, py, px, py * NX + px).wait_recv())

    def wave_z(to, owner):
        return remote(
            wave_row.at[0:1, :], wave_mid.at[owner, 0:1, :],
            z_send.at[chunks, to], z_recv.at[chunks, owner], peer_at(y, to, x),
        )

    wave_z_own = pltpu.make_async_copy(
        wave_row.at[0:1, :], wave_mid.at[z, 0:1, :], own_sem.at[0, chunks]
    )

    def wave_p(py, px, owner):
        return remote(
            wave_mid.at[:, 0:1, :], wave_all.at[owner, :, 0:1, :],
            p_send.at[chunks, py * NX + px], p_recv.at[chunks, owner], peer_at(py, z, px),
        )

    wave_p_own = pltpu.make_async_copy(
        wave_mid.at[:, 0:1, :], wave_all.at[place, :, 0:1, :], own_sem.at[1, chunks]
    )

    def load(slot):
        return (
            pltpu.make_async_copy(spectral_hbm.at[slot], spectral.at[slot], load_sem.at[0, slot]),
            pltpu.make_async_copy(legendre_hbm.at[slot], legendre.at[slot], load_sem.at[1, slot]),
        )

    def start_load(c):
        for slot in (2 * c, 2 * c + 1):
            for copy in load(slot):
                copy.start()

    first_order = (0, 3, 1, 4, 2)
    start_load(first_order[0])

    barrier = pltpu.get_barrier_semaphore()

    def greet(peer):
        pl.semaphore_signal(
            barrier, inc=1, device_id={"wa": peer}, device_id_type=pl.DeviceIdType.MESH
        )

    each_z(lambda to: greet(peer_at(y, to, x)))
    each_place(lambda py, px: greet(peer_at(py, z, px)))
    at_slot = lax.broadcasted_iota(jnp.int32, wave_row.shape, 1)
    waves = jnp.zeros(wave_row.shape, jnp.int32)
    for slot in range(slots):
        waves = jnp.where(at_slot == slot, wave_smem[slot], waves)
    wave_row[...] = waves
    staged[...] = jnp.zeros(staged.shape, jnp.float32)

    index = lax.broadcasted_iota(jnp.int32, (1, degrees), 1)

    def sums_of(slot):
        offset = index - wave_smem[slot]
        keep = jnp.where(offset >= 0, 1.0, 0.0)
        flip = jnp.where((offset & 1) == 0, keep, -keep)
        coeff = spectral[slot]
        both = jnp.concatenate(
            [coeff * keep.astype(coeff.dtype), coeff * flip.astype(coeff.dtype)], 0
        )
        return jnp.dot(both, legendre[slot], preferred_element_type=jnp.float32)

    def synthesize(c):
        first = sums_of(2 * c)
        second = sums_of(2 * c + 1)
        for side in range(2):
            part = slice(side * columns, (side + 1) * columns)
            staged[side, 0:north, :] = jnp.concatenate([first[part], second[part]], 0).T
            for slab in range(OWNERS // 2):
                d = OWNERS - 1 - slab if side else slab
                send[c, d // (NZ * NX), (d // NX) % NZ, d % NX] = staged[
                    side, rows * slab:rows * slab + 8, :
                ]

    for c in first_order:
        for slot in (2 * c, 2 * c + 1):
            for copy in load(slot):
                copy.wait()
        if c == first_order[0]:
            for other in first_order[1:]:
                start_load(other)
        synthesize(c)
        if c == first_order[0]:
            pl.semaphore_wait(barrier, NZ - 1 + PLANE - 1)
            each_z(lambda to: wave_z(to, z).start())
            wave_z_own.start()
        if c < line_first:
            start_z(c)
        else:
            start_p(c)

    wave_z_own.wait()
    each_z(lambda to: wave_z(to, to).wait_recv())
    each_place(lambda py, px: wave_p(py, px, place).start())
    wave_p_own.start()
    even[...] = jnp.zeros(even.shape, jnp.float32)
    odd[...] = jnp.zeros(odd.shape, jnp.float32)

    wave_p_own.wait()
    each_place(lambda py, px: wave_p(py, px, py * NX + px).wait_recv())
    flat_waves = wave_all.reshape(OWNERS * 8, LANES)
    gathered = flat_waves[pl.ds(0, OWNERS, stride=8), :].astype(jnp.float32)
    for slot in range(slots):
        wave_rows[slot * OWNERS:(slot + 1) * OWNERS, :] = jnp.broadcast_to(
            gathered[:, slot:slot + 1], (OWNERS, LANES)
        )
    position = lax.broadcasted_iota(jnp.int32, (1, LANES), 1).astype(jnp.float32)
    sin_tiles = sin_hi.shape[1] // LANES

    def fill(i, carry):
        at = pl.ds(pl.multiple_of(i * 16, 16), 16)
        waves = wave_rows[at, :]
        weight = jnp.where(waves == 0.0, 1.0, 2.0)
        c, s = cos_sin(waves * position)
        turn_c, turn_s = cos_sin(waves * float(LANES))
        c, s = c * weight, s * weight
        for tile in range(sin_tiles + 1):
            to = slice(tile * LANES, (tile + 1) * LANES)
            top = c.astype(jnp.bfloat16)
            cos_hi[at, to] = top
            cos_lo[at, to] = (c - top.astype(jnp.float32)).astype(jnp.bfloat16)
            if tile < sin_tiles:
                top = s.astype(jnp.bfloat16)
                sin_hi[at, to] = top
                sin_lo[at, to] = (s - top.astype(jnp.float32)).astype(jnp.bfloat16)
                c, s = c * turn_c - s * turn_s, s * turn_c + c * turn_s
        return carry

    south = me // (OWNERS // 2)
    flat = recv.reshape(chunks * OWNERS * 8, LANES)

    def add_chunk(c):
        parts = [[], []]
        for row in range(rows):
            source = row + south * (rows - 1 - 2 * row)
            turned = flat[pl.ds(c * OWNERS * 8 + source, OWNERS, stride=8), :].T
            for part in range(2):
                parts[part].append(
                    jnp.concatenate(
                        [turned[part * levels:(part + 1) * levels],
                         turned[(2 + part) * levels:(3 + part) * levels]], 1
                    )
                )
        at = pl.ds(pl.multiple_of(c * 2 * OWNERS, 2 * OWNERS), 2 * OWNERS)
        for part, total, high, low in ((0, even, cos_hi, cos_lo), (1, odd, sin_hi, sin_lo)):
            values = jnp.concatenate(parts[part], 0)
            top = values.astype(jnp.bfloat16)
            rest = (values - top.astype(jnp.float32)).astype(jnp.bfloat16)
            table = high[at, :]
            sums = jnp.dot(top, table, preferred_element_type=jnp.float32)
            sums += jnp.dot(rest, table, preferred_element_type=jnp.float32)
            sums += jnp.dot(top, low[at, :], preferred_element_type=jnp.float32)
            total[...] += sums

    wait_z(0)
    start_p(0)
    lax.fori_loop(0, wave_rows.shape[0] // 16, fill, 0)
    for c in range(1, line_first):
        wait_z(c)
        start_p(c)
        if line_first - 1 + c < chunks:
            wait_p(line_first - 1 + c)
            start_z(line_first - 1 + c)
        wait_p(c - 1)
        add_chunk(c - 1)
    wait_p(line_first - 1)
    add_chunk(line_first - 1)
    for c in range(line_first, chunks):
        wait_z(c)
        add_chunk(c)

    r = lax.broadcasted_iota(jnp.int32, (TILE, TILE), 0)
    q = lax.broadcasted_iota(jnp.int32, (TILE, TILE), 1)
    mirror = jnp.where(r + q == TILE, 1.0, 0.0).astype(jnp.bfloat16)
    at_zero = lax.broadcasted_iota(jnp.int32, (1, TILE), 1) == 0
    tiles = odd.shape[1] // TILE
    after = even[:, tiles * TILE:tiles * TILE + 1]
    for tile in range(tiles - 1, -1, -1):
        to = slice(tile * TILE, (tile + 1) * TILE)
        back = slice((2 * tiles - 1 - tile) * TILE, (2 * tiles - tile) * TILE)
        e, o = even[:, to], odd[:, to]
        out[:, :, to] = (e - o).reshape(rows, levels, TILE)
        d = e + o
        top = d.astype(jnp.bfloat16)
        rest = (d - top.astype(jnp.float32)).astype(jnp.bfloat16)
        turned = jnp.dot(top, mirror, preferred_element_type=jnp.float32)
        turned += jnp.dot(rest, mirror, preferred_element_type=jnp.float32)
        out[:, :, back] = jnp.where(at_zero, after, turned).reshape(rows, levels, TILE)
        after = d[:, 0:1]

    each_z(lambda to: wave_z(to, z).wait_send())
    each_place(lambda py, px: wave_p(py, px, place).wait_send())

    for c in range(chunks):
        each_z(lambda to: z_copy(c, to, z).wait_send())
        each_place(lambda py, px: p_copy(c, py, px, place).wait_send())


def on_device(spectral, legendre, wavenumber):
    slots, degrees, _, levels = spectral.shape
    north = legendre.shape[2]
    rows = 2 * north // OWNERS
    chunks = slots // 2
    line_first = 3
    coeff = jnp.transpose(spectral, (0, 2, 3, 1)).reshape(slots, 2 * levels, degrees)
    depth = slots * OWNERS
    half = NLON // 2
    f32, bf16, i32 = jnp.float32, jnp.bfloat16, jnp.int32
    grid = pl.pallas_call(
        functools.partial(transform_kernel, chunks, line_first, rows),
        out_shape=pltpu.VMEM((rows, levels, NLON), f32),
        in_specs=[
            pl.BlockSpec(memory_space=pltpu.SMEM),
            pl.BlockSpec(memory_space=pltpu.HBM),
            pl.BlockSpec(memory_space=pltpu.HBM),
        ],
        out_specs=pl.BlockSpec(memory_space=pltpu.VMEM),
        scratch_shapes=[
            pltpu.VMEM((slots, 2 * levels, degrees), bf16),
            pltpu.VMEM((slots, degrees, north), bf16),
            pltpu.VMEM((2, north + 8, LANES), f32),
            pltpu.VMEM((chunks, NY, NZ, NX, 8, LANES), f32),
            pltpu.VMEM((line_first, NZ, NY, NX, 8, LANES), f32),
            pltpu.VMEM((chunks - line_first, PLANE, NZ, 8, LANES), f32),
            pltpu.VMEM((chunks, PLANE, NZ, 8, LANES), f32),
            pltpu.VMEM((8, LANES), i32),
            pltpu.VMEM((NZ, 8, LANES), i32),
            pltpu.VMEM((PLANE, NZ, 8, LANES), i32),
            pltpu.VMEM((depth, LANES), f32),
            pltpu.VMEM((depth, half + LANES), bf16),
            pltpu.VMEM((depth, half + LANES), bf16),
            pltpu.VMEM((depth, half), bf16),
            pltpu.VMEM((depth, half), bf16),
            pltpu.VMEM((rows * levels, half + LANES), f32),
            pltpu.VMEM((rows * levels, half), f32),
            pltpu.SemaphoreType.DMA((2, slots)),
            pltpu.SemaphoreType.DMA((chunks + 1, NZ)),
            pltpu.SemaphoreType.DMA((chunks + 1, NZ)),
            pltpu.SemaphoreType.DMA((chunks + 1, PLANE)),
            pltpu.SemaphoreType.DMA((chunks + 1, PLANE)),
            pltpu.SemaphoreType.DMA((2, chunks + 1)),
        ],
        compiler_params=pltpu.CompilerParams(
            collective_id=0, has_side_effects=True, vmem_limit_bytes=56 * 2**20,
        ),
    )(wavenumber, coeff, legendre)
    return jnp.transpose(grid, (0, 2, 1))


def solution(mesh):
    return jax.shard_map(
        on_device,
        mesh=mesh,
        in_specs=(P("wa", None, None, "lev"), P("wa", None, None), P("wa")),
        out_specs=P("wa", None, "lev"),
        check_vma=False,
    )
```

```python
import functools
import math

import jax
import jax.numpy as jnp
from jax import lax
from jax.experimental import pallas as pl
from jax.experimental.pallas import tpu as pltpu
from jax.sharding import PartitionSpec as P

NLON = 2560
TILE = 256
LANES = 128
NY, NZ, NX = 4, 8, 4
PLANE = NY * NX
OWNERS = NY * NZ * NX


def cos_sin(turns):
    quarter = jnp.floor(turns * (4.0 / NLON) + 0.5)
    x = (turns - quarter * (NLON // 4)) * (2.0 * math.pi / NLON)
    y = x * x
    s = x * (1.0 + y * (-1 / 6 + y * (1 / 120 + y * (-1 / 5040 + y * (1 / 362880)))))
    c = 1.0 + y * (-1 / 2 + y * (1 / 24 + y * (-1 / 720 + y * (1 / 40320 - y * (1 / 3628800)))))
    which = quarter.astype(jnp.int32) & 3
    odd = (which & 1) == 1
    cos_out = jnp.where(odd, s, c)
    sin_out = jnp.where(odd, c, s)
    cos_out = jnp.where((which == 1) | (which == 2), -cos_out, cos_out)
    sin_out = jnp.where(which >= 2, -sin_out, sin_out)
    return cos_out, sin_out


def transform_kernel(
    chunks, line_first, groups, rows,
    wave_smem, spectral_hbm, legendre_hbm,
    out,
    spectral, legendre, staged, send, middle, spread, recv,
    wave_row, wave_mid, wave_all, wave_rows,
    cos_hi, cos_lo, sin_hi, sin_lo, even, odd,
    load_sem, z_send, z_recv, p_send, p_recv, own_sem,
):
    me = lax.axis_index("wa")
    y, z, x = me // (NZ * NX), (me // NX) % NZ, me % NX
    place = y * NX + x
    slots, columns, degrees = spectral.shape
    north = legendre.shape[2]
    levels = columns // 2

    def peer_at(py, pz, px):
        return (py * NZ + pz) * NX + px

    def remote(src, dst, send_sem, recv_sem, peer):
        return pltpu.make_async_remote_copy(
            src_ref=src, dst_ref=dst, send_sem=send_sem, recv_sem=recv_sem,
            device_id={"wa": peer}, device_id_type=pl.DeviceIdType.MESH,
        )

    def each_z(act):
        for d in (4, 3, 5, 2, 6, 1, 7):
            act((z + d) % NZ)

    def each_place(act):
        for d in (5, 15, 7, 13, 10, 6, 9, 14, 11, 2, 8, 1, 4, 3, 12):
            act((y + d // NX) % NY, (x + d % NX) % NX)

    def z_views(c, g, to, owner):
        if c < line_first:
            return send.at[c, :, to, :, 0:rows, :], middle.at[c, owner, :, :, 0:rows, :]
        part = slice(g * rows // groups, (g + 1) * rows // groups) if c == chunks - 1 else slice(0, rows)
        return spread.at[c - line_first, :, to, part, :], recv.at[c, :, owner, part, :]

    def z_copy(c, g, to, owner):
        src, dst = z_views(c, g, to, owner)
        return remote(src, dst, z_send.at[c + g], z_recv.at[c + g], peer_at(y, to, x))

    def z_own(c, g):
        src, dst = z_views(c, g, z, z)
        return pltpu.make_async_copy(src, dst, own_sem.at[0, c + g])

    def z_all(c, g):
        if c < line_first:
            landed = middle.at[c, 0:NZ - 1, :, :, 0:rows, :]
        else:
            part = slice(g * rows // groups, (g + 1) * rows // groups) if c == chunks - 1 else slice(0, rows)
            landed = recv.at[c, :, 0:NZ - 1, part, :]
        return remote(landed, landed, z_send.at[c + g], z_recv.at[c + g], peer_at(y, (z + 1) % NZ, x))

    def p_all(c):
        if c < line_first:
            landed = recv.at[c, 0:PLANE - 1, :, 0:rows, :]
        else:
            landed = spread.at[c - line_first, 0:PLANE - 1, :, 0:rows, :]
        return remote(landed, landed, p_send.at[c], p_recv.at[c], peer_at(y, z, (x + 1) % NX))

    def groups_of(c):
        return range(groups if c == chunks - 1 else 1)

    def p_copy(c, py, px, owner):
        if c < line_first:
            src, dst = middle.at[c, :, py, px, 0:rows, :], recv.at[c, owner, :, 0:rows, :]
        else:
            src = send.at[c, py, :, px, 0:rows, :]
            dst = spread.at[c - line_first, owner, :, 0:rows, :]
        return remote(
            src, dst, p_send.at[c], p_recv.at[c], peer_at(py, z, px)
        )

    def p_own(c):
        if c < line_first:
            src, dst = middle.at[c, :, y, x, 0:rows, :], recv.at[c, place, :, 0:rows, :]
        else:
            src = send.at[c, y, :, x, 0:rows, :]
            dst = spread.at[c - line_first, place, :, 0:rows, :]
        return pltpu.make_async_copy(src, dst, own_sem.at[1, c])

    def start_z(c):
        for g in groups_of(c):
            each_z(lambda to: z_copy(c, g, to, z).start())
            z_own(c, g).start()

    def start_p(c):
        each_place(lambda py, px: p_copy(c, py, px, place).start())
        p_own(c).start()

    def wait_z(c, g=0):
        z_own(c, g).wait()
        z_all(c, g).wait_recv()

    def wait_p(c):
        p_own(c).wait()
        p_all(c).wait_recv()

    wave_job = chunks - 1 + groups

    def wave_z(to, owner):
        return remote(
            wave_row.at[0:1, :], wave_mid.at[owner, 0:1, :],
            z_send.at[wave_job], z_recv.at[wave_job], peer_at(y, to, x),
        )

    wave_z_own = pltpu.make_async_copy(
        wave_row.at[0:1, :], wave_mid.at[z, 0:1, :], own_sem.at[0, wave_job]
    )

    def wave_p(py, px, owner):
        return remote(
            wave_mid.at[:, 0:1, :], wave_all.at[owner, :, 0:1, :],
            p_send.at[chunks], p_recv.at[chunks], peer_at(py, z, px),
        )

    wave_z_all = remote(
        wave_mid.at[0:NZ - 1, 0:1, :], wave_mid.at[0:NZ - 1, 0:1, :],
        z_send.at[wave_job], z_recv.at[wave_job], peer_at(y, (z + 1) % NZ, x),
    )
    wave_p_all = remote(
        wave_all.at[0:PLANE - 1, :, 0:1, :], wave_all.at[0:PLANE - 1, :, 0:1, :],
        p_send.at[chunks], p_recv.at[chunks], peer_at(y, z, (x + 1) % NX),
    )
    wave_p_own = pltpu.make_async_copy(
        wave_mid.at[:, 0:1, :], wave_all.at[place, :, 0:1, :], own_sem.at[1, chunks]
    )

    def load(c):
        pair = slice(2 * c, 2 * c + 2)
        return (
            pltpu.make_async_copy(spectral_hbm.at[pair], spectral.at[pair], load_sem.at[0, c]),
            pltpu.make_async_copy(legendre_hbm.at[pair], legendre.at[pair], load_sem.at[1, c]),
        )

    def start_load(c):
        for copy in load(c):
            copy.start()

    first_order = (0, 3, 1, 4, 2)
    start_load(first_order[0])

    barrier = pltpu.get_barrier_semaphore()

    def greet(peer):
        pl.semaphore_signal(
            barrier, inc=1, device_id={"wa": peer}, device_id_type=pl.DeviceIdType.MESH
        )

    each_z(lambda to: greet(peer_at(y, to, x)))
    each_place(lambda py, px: greet(peer_at(py, z, px)))
    at_slot = lax.broadcasted_iota(jnp.int32, wave_row.shape, 1)
    waves = jnp.zeros(wave_row.shape, jnp.int32)
    for slot in range(slots):
        waves = jnp.where(at_slot == slot, wave_smem[slot], waves)
    wave_row[...] = waves
    staged[...] = jnp.zeros(staged.shape, jnp.float32)

    index = lax.broadcasted_iota(jnp.int32, (1, degrees), 1)

    def sums_of(slot):
        offset = index - wave_smem[slot]
        keep = jnp.where(offset >= 0, 1.0, 0.0)
        flip = jnp.where((offset & 1) == 0, keep, -keep)
        coeff = spectral[slot]
        both = jnp.concatenate(
            [coeff * keep.astype(coeff.dtype), coeff * flip.astype(coeff.dtype)], 0
        )
        return jnp.dot(both, legendre[slot], preferred_element_type=jnp.float32)

    def synthesize(c):
        first = sums_of(2 * c)
        second = sums_of(2 * c + 1)
        for side in range(2):
            part = slice(side * columns, (side + 1) * columns)
            staged[side, 0:north, :] = jnp.concatenate([first[part], second[part]], 0).T
            for slab in range(OWNERS // 2):
                d = OWNERS - 1 - slab if side else slab
                send[c, d // (NZ * NX), (d // NX) % NZ, d % NX] = staged[
                    side, rows * slab:rows * slab + 8, :
                ]

    for c in first_order:
        for copy in load(c):
            copy.wait()
        if c == first_order[0]:
            for other in first_order[1:]:
                start_load(other)
        synthesize(c)
        if c == first_order[0]:
            pl.semaphore_wait(barrier, NZ - 1 + PLANE - 1)
            each_z(lambda to: wave_z(to, z).start())
            wave_z_own.start()
        if c < line_first:
            start_z(c)

    wave_z_own.wait()
    wave_z_all.wait_recv()
    each_place(lambda py, px: wave_p(py, px, place).start())
    wave_p_own.start()
    for c in range(line_first, chunks):
        start_p(c)
    even[...] = jnp.zeros(even.shape, jnp.float32)
    odd[...] = jnp.zeros(odd.shape, jnp.float32)

    def drain_z(c):
        for g in groups_of(c):
            z_all(c, g).wait_send()

    def drain_p(c):
        p_all(c).wait_send()

    wait_z(0)
    start_p(0)
    wave_p_own.wait()
    wave_p_all.wait_recv()
    flat_waves = wave_all.reshape(OWNERS * 8, LANES)
    gathered = flat_waves[pl.ds(0, OWNERS, stride=8), :].astype(jnp.float32)
    for slot in range(slots):
        wave_rows[slot * OWNERS:(slot + 1) * OWNERS, :] = jnp.broadcast_to(
            gathered[:, slot:slot + 1], (OWNERS, LANES)
        )
    position = lax.broadcasted_iota(jnp.int32, (1, LANES), 1).astype(jnp.float32)
    sin_tiles = sin_hi.shape[1] // LANES

    def fill(i, carry):
        at = pl.ds(pl.multiple_of(i * 16, 16), 16)
        waves = wave_rows[at, :]
        weight = jnp.where(waves == 0.0, 1.0, 2.0)
        c, s = cos_sin(waves * position)
        turn_c, turn_s = cos_sin(waves * float(LANES))
        c, s = c * weight, s * weight
        for tile in range(sin_tiles + 1):
            to = slice(tile * LANES, (tile + 1) * LANES)
            top = c.astype(jnp.bfloat16)
            cos_hi[at, to] = top
            cos_lo[at, to] = (c - top.astype(jnp.float32)).astype(jnp.bfloat16)
            if tile < sin_tiles:
                top = s.astype(jnp.bfloat16)
                sin_hi[at, to] = top
                sin_lo[at, to] = (s - top.astype(jnp.float32)).astype(jnp.bfloat16)
                c, s = c * turn_c - s * turn_s, s * turn_c + c * turn_s
        return carry

    south = me // (OWNERS // 2)
    flat = recv.reshape(chunks * OWNERS * 8, LANES)

    def add_chunk(c, low_row=0, high_row=rows):
        parts = [[], []]
        for row in range(low_row, high_row):
            turned = flat[pl.ds(c * OWNERS * 8 + row, OWNERS, stride=8), :].T
            for part in range(2):
                parts[part].append(
                    jnp.concatenate(
                        [turned[part * levels:(part + 1) * levels],
                         turned[(2 + part) * levels:(3 + part) * levels]], 1
                    )
                )
        at = pl.ds(pl.multiple_of(c * 2 * OWNERS, 2 * OWNERS), 2 * OWNERS)
        for part, total, high, low in ((0, even, cos_hi, cos_lo), (1, odd, sin_hi, sin_lo)):
            values = jnp.concatenate(parts[part], 0)
            top = values.astype(jnp.bfloat16)
            rest = (values - top.astype(jnp.float32)).astype(jnp.bfloat16)
            table = high[at, :]
            sums = jnp.dot(top, table, preferred_element_type=jnp.float32)
            sums += jnp.dot(rest, table, preferred_element_type=jnp.float32)
            sums += jnp.dot(top, low[at, :], preferred_element_type=jnp.float32)
            total[low_row * levels:high_row * levels, :] += sums

    lax.fori_loop(0, wave_rows.shape[0] // 16, fill, 0)
    for c in range(1, line_first):
        if c == line_first - 1:
            wave_z_all.wait_send()
            wave_p_all.wait_send()
            drain_z(0)
            drain_p(line_first)
            drain_p(line_first + 1)
        wait_z(c)
        start_p(c)
        if line_first - 1 + c < chunks:
            wait_p(line_first - 1 + c)
            start_z(line_first - 1 + c)
        wait_p(c - 1)
        add_chunk(c - 1)
    wait_p(line_first - 1)
    add_chunk(line_first - 1)
    for c in range(line_first, chunks - 1):
        wait_z(c)
        add_chunk(c)

    r = lax.broadcasted_iota(jnp.int32, (TILE, TILE), 0)
    q = lax.broadcasted_iota(jnp.int32, (TILE, TILE), 1)
    mirror = jnp.where(r + q == TILE, 1.0, 0.0).astype(jnp.bfloat16)
    at_zero = lax.broadcasted_iota(jnp.int32, (1, TILE), 1) == 0
    tiles = odd.shape[1] // TILE

    def finish(low_row, high_row):
        at = slice(low_row * levels, high_row * levels)

        def put(values, to):
            for row in range(low_row, high_row):
                target = row + south * (rows - 1 - 2 * row)
                out[target, :, to] = values[(row - low_row) * levels:(row - low_row + 1) * levels]

        after = even[at, tiles * TILE:tiles * TILE + 1]
        for tile in range(tiles - 1, -1, -1):
            to = slice(tile * TILE, (tile + 1) * TILE)
            back = slice((2 * tiles - 1 - tile) * TILE, (2 * tiles - tile) * TILE)
            e, o = even[at, to], odd[at, to]
            put(e - o, to)
            d = e + o
            top = d.astype(jnp.bfloat16)
            rest = (d - top.astype(jnp.float32)).astype(jnp.bfloat16)
            turned = jnp.dot(top, mirror, preferred_element_type=jnp.float32)
            turned += jnp.dot(rest, mirror, preferred_element_type=jnp.float32)
            put(jnp.where(at_zero, after, turned), back)
            after = d[:, 0:1]

    for c in range(1, chunks - 1):
        drain_z(c)
    for c in range(line_first):
        drain_p(c)
    for g in range(groups):
        wait_z(chunks - 1, g)
        low_row, high_row = g * rows // groups, (g + 1) * rows // groups
        add_chunk(chunks - 1, low_row, high_row)
        finish(low_row, high_row)

    drain_z(chunks - 1)


def on_device(spectral, legendre, wavenumber):
    slots, degrees, _, levels = spectral.shape
    north = legendre.shape[2]
    rows = 2 * north // OWNERS
    chunks = slots // 2
    line_first = 3
    groups = 2
    coeff = jnp.transpose(spectral, (0, 2, 3, 1)).reshape(slots, 2 * levels, degrees)
    depth = slots * OWNERS
    half = NLON // 2
    f32, bf16, i32 = jnp.float32, jnp.bfloat16, jnp.int32
    grid = pl.pallas_call(
        functools.partial(transform_kernel, chunks, line_first, groups, rows),
        out_shape=pltpu.VMEM((rows, levels, NLON), f32),
        in_specs=[
            pl.BlockSpec(memory_space=pltpu.SMEM),
            pl.BlockSpec(memory_space=pltpu.HBM),
            pl.BlockSpec(memory_space=pltpu.HBM),
        ],
        out_specs=pl.BlockSpec(memory_space=pltpu.VMEM),
        scratch_shapes=[
            pltpu.VMEM((slots, 2 * levels, degrees), bf16),
            pltpu.VMEM((slots, degrees, north), bf16),
            pltpu.VMEM((2, north + 8, LANES), f32),
            pltpu.VMEM((chunks, NY, NZ, NX, 8, LANES), f32),
            pltpu.VMEM((line_first, NZ, NY, NX, 8, LANES), f32),
            pltpu.VMEM((chunks - line_first, PLANE, NZ, 8, LANES), f32),
            pltpu.VMEM((chunks, PLANE, NZ, 8, LANES), f32),
            pltpu.VMEM((8, LANES), i32),
            pltpu.VMEM((NZ, 8, LANES), i32),
            pltpu.VMEM((PLANE, NZ, 8, LANES), i32),
            pltpu.VMEM((depth, LANES), f32),
            pltpu.VMEM((depth, half + LANES), bf16),
            pltpu.VMEM((depth, half + LANES), bf16),
            pltpu.VMEM((depth, half), bf16),
            pltpu.VMEM((depth, half), bf16),
            pltpu.VMEM((rows * levels, half + LANES), f32),
            pltpu.VMEM((rows * levels, half), f32),
            pltpu.SemaphoreType.DMA((2, chunks)),
            pltpu.SemaphoreType.DMA((chunks + groups,)),
            pltpu.SemaphoreType.DMA((chunks + groups,)),
            pltpu.SemaphoreType.DMA((chunks + 1,)),
            pltpu.SemaphoreType.DMA((chunks + 1,)),
            pltpu.SemaphoreType.DMA((2, chunks + groups)),
        ],
        compiler_params=pltpu.CompilerParams(
            collective_id=0, has_side_effects=True, vmem_limit_bytes=56 * 2**20,
        ),
    )(wavenumber, coeff, legendre)
    return jnp.transpose(grid, (0, 2, 1))


def solution(mesh):
    return jax.shard_map(
        on_device,
        mesh=mesh,
        in_specs=(P("wa", None, None, "lev"), P("wa", None, None), P("wa")),
        out_specs=P("wa", None, "lev"),
        check_vma=False,
    )
```

```python
import functools
import math

import jax
import jax.numpy as jnp
from jax import lax
from jax.experimental import pallas as pl
from jax.experimental.pallas import tpu as pltpu
from jax.sharding import PartitionSpec as P

NLON = 2560
TILE = 256
LANES = 128
NY, NZ, NX = 4, 8, 4
PLANE = NY * NX
OWNERS = NY * NZ * NX


def cos_sin(turns):
    quarter = jnp.floor(turns * (4.0 / NLON) + 0.5)
    x = (turns - quarter * (NLON // 4)) * (2.0 * math.pi / NLON)
    y = x * x
    s = x * (1.0 + y * (-1 / 6 + y * (1 / 120 + y * (-1 / 5040 + y * (1 / 362880)))))
    c = 1.0 + y * (-1 / 2 + y * (1 / 24 + y * (-1 / 720 + y * (1 / 40320 - y * (1 / 3628800)))))
    which = quarter.astype(jnp.int32) & 3
    odd = (which & 1) == 1
    cos_out = jnp.where(odd, s, c)
    sin_out = jnp.where(odd, c, s)
    cos_out = jnp.where((which == 1) | (which == 2), -cos_out, cos_out)
    sin_out = jnp.where(which >= 2, -sin_out, sin_out)
    return cos_out, sin_out


def transform_kernel(
    chunks, line_first, groups, rows,
    wave_hbm, spectral_hbm, legendre_hbm,
    out,
    wave_smem, spectral, legendre, staged, send, middle, spread, recv,
    wave_row, wave_mid, wave_all, wave_rows,
    cos_hi, cos_lo, sin_hi, sin_lo, even, odd,
    load_sem, z_send, z_recv, p_send, p_recv, own_sem, wave_sem,
):
    me = lax.axis_index("wa")
    y, z, x = me // (NZ * NX), (me // NX) % NZ, me % NX
    place = y * NX + x
    slots, columns, degrees = spectral.shape
    north = legendre.shape[2]
    levels = columns // 2

    def peer_at(py, pz, px):
        return (py * NZ + pz) * NX + px

    def remote(src, dst, send_sem, recv_sem, peer):
        return pltpu.make_async_remote_copy(
            src_ref=src, dst_ref=dst, send_sem=send_sem, recv_sem=recv_sem,
            device_id={"wa": peer}, device_id_type=pl.DeviceIdType.MESH,
        )

    def each_z(act):
        for d in (4, 3, 5, 2, 6, 1, 7):
            act((z + d) % NZ)

    def each_place(act):
        for d in (5, 15, 7, 13, 10, 6, 9, 14, 11, 2, 8, 1, 4, 3, 12):
            act((y + d // NX) % NY, (x + d % NX) % NX)

    def z_views(c, g, to, owner):
        if c < line_first:
            return send.at[c, :, to, :, 0:rows, :], middle.at[c, owner, :, :, 0:rows, :]
        part = slice(g * rows // groups, (g + 1) * rows // groups) if c == chunks - 1 else slice(0, rows)
        return spread.at[c - line_first, :, to, part, :], recv.at[c, :, owner, part, :]

    def z_copy(c, g, to, owner):
        src, dst = z_views(c, g, to, owner)
        return remote(src, dst, z_send.at[c + g], z_recv.at[c + g], peer_at(y, to, x))

    def z_own(c, g):
        src, dst = z_views(c, g, z, z)
        return pltpu.make_async_copy(src, dst, own_sem.at[0, c + g])

    def z_all(c, g):
        if c < line_first:
            landed = middle.at[c, 0:NZ - 1, :, :, 0:rows, :]
        else:
            part = slice(g * rows // groups, (g + 1) * rows // groups) if c == chunks - 1 else slice(0, rows)
            landed = recv.at[c, :, 0:NZ - 1, part, :]
        return remote(landed, landed, z_send.at[c + g], z_recv.at[c + g], peer_at(y, (z + 1) % NZ, x))

    def p_all(c):
        if c < line_first:
            landed = recv.at[c, 0:PLANE - 1, :, 0:rows, :]
        else:
            landed = spread.at[c - line_first, 0:PLANE - 1, :, 0:rows, :]
        return remote(landed, landed, p_send.at[c], p_recv.at[c], peer_at(y, z, (x + 1) % NX))

    def groups_of(c):
        return range(groups if c == chunks - 1 else 1)

    def p_copy(c, py, px, owner):
        if c < line_first:
            src, dst = middle.at[c, :, py, px, 0:rows, :], recv.at[c, owner, :, 0:rows, :]
        else:
            src = send.at[c, py, :, px, 0:rows, :]
            dst = spread.at[c - line_first, owner, :, 0:rows, :]
        return remote(
            src, dst, p_send.at[c], p_recv.at[c], peer_at(py, z, px)
        )

    def p_own(c):
        if c < line_first:
            src, dst = middle.at[c, :, y, x, 0:rows, :], recv.at[c, place, :, 0:rows, :]
        else:
            src = send.at[c, y, :, x, 0:rows, :]
            dst = spread.at[c - line_first, place, :, 0:rows, :]
        return pltpu.make_async_copy(src, dst, own_sem.at[1, c])

    def start_z(c):
        for g in groups_of(c):
            each_z(lambda to: z_copy(c, g, to, z).start())
            z_own(c, g).start()

    def start_p(c):
        each_place(lambda py, px: p_copy(c, py, px, place).start())
        p_own(c).start()

    def wait_z(c, g=0):
        z_own(c, g).wait()
        z_all(c, g).wait_recv()

    def wait_p(c):
        p_own(c).wait()
        p_all(c).wait_recv()

    wave_job = chunks - 1 + groups

    def wave_z(to, owner):
        return remote(
            wave_row.at[0:1, :], wave_mid.at[owner, 0:1, :],
            z_send.at[wave_job], z_recv.at[wave_job], peer_at(y, to, x),
        )

    wave_z_own = pltpu.make_async_copy(
        wave_row.at[0:1, :], wave_mid.at[z, 0:1, :], own_sem.at[0, wave_job]
    )

    def wave_p(py, px, owner):
        return remote(
            wave_mid.at[:, 0:1, :], wave_all.at[owner, :, 0:1, :],
            p_send.at[chunks], p_recv.at[chunks], peer_at(py, z, px),
        )

    wave_z_all = remote(
        wave_mid.at[0:NZ - 1, 0:1, :], wave_mid.at[0:NZ - 1, 0:1, :],
        z_send.at[wave_job], z_recv.at[wave_job], peer_at(y, (z + 1) % NZ, x),
    )
    wave_p_all = remote(
        wave_all.at[0:PLANE - 1, :, 0:1, :], wave_all.at[0:PLANE - 1, :, 0:1, :],
        p_send.at[chunks], p_recv.at[chunks], peer_at(y, z, (x + 1) % NX),
    )
    wave_p_own = pltpu.make_async_copy(
        wave_mid.at[:, 0:1, :], wave_all.at[place, :, 0:1, :], own_sem.at[1, chunks]
    )

    def load(c):
        pair = slice(2 * c, 2 * c + 2)
        return (
            pltpu.make_async_copy(spectral_hbm.at[pair], spectral.at[pair], load_sem.at[0, c]),
            pltpu.make_async_copy(legendre_hbm.at[pair], legendre.at[pair], load_sem.at[1, c]),
        )

    def start_load(c):
        for copy in load(c):
            copy.start()

    first_order = (0, 3, 1, 4, 2)
    own_waves = pltpu.make_async_copy(wave_hbm, wave_smem, wave_sem)
    own_waves.start()
    start_load(first_order[0])

    barrier = pltpu.get_barrier_semaphore()

    def greet(peer):
        pl.semaphore_signal(
            barrier, inc=1, device_id={"wa": peer}, device_id_type=pl.DeviceIdType.MESH
        )

    each_z(lambda to: greet(peer_at(y, to, x)))
    each_place(lambda py, px: greet(peer_at(py, z, px)))
    own_waves.wait()
    at_slot = lax.broadcasted_iota(jnp.int32, wave_row.shape, 1)
    waves = jnp.zeros(wave_row.shape, jnp.int32)
    for slot in range(slots):
        waves = jnp.where(at_slot == slot, wave_smem[slot], waves)
    wave_row[...] = waves
    staged[...] = jnp.zeros(staged.shape, jnp.float32)

    index = lax.broadcasted_iota(jnp.int32, (1, degrees), 1)

    def sums_of(slot):
        offset = index - wave_smem[slot]
        keep = jnp.where(offset >= 0, 1.0, 0.0)
        flip = jnp.where((offset & 1) == 0, keep, -keep)
        coeff = spectral[slot]
        both = jnp.concatenate(
            [coeff * keep.astype(coeff.dtype), coeff * flip.astype(coeff.dtype)], 0
        )
        return jnp.dot(both, legendre[slot], preferred_element_type=jnp.float32)

    def synthesize(c):
        first = sums_of(2 * c)
        second = sums_of(2 * c + 1)
        for side in range(2):
            part = slice(side * columns, (side + 1) * columns)
            staged[side, 0:north, :] = jnp.concatenate([first[part], second[part]], 0).T
            for slab in range(OWNERS // 2):
                d = OWNERS - 1 - slab if side else slab
                send[c, d // (NZ * NX), (d // NX) % NZ, d % NX] = staged[
                    side, rows * slab:rows * slab + 8, :
                ]

    for c in first_order:
        for copy in load(c):
            copy.wait()
        if c == first_order[0]:
            for other in first_order[1:]:
                start_load(other)
        synthesize(c)
        if c == first_order[0]:
            pl.semaphore_wait(barrier, NZ - 1 + PLANE - 1)
            each_z(lambda to: wave_z(to, z).start())
            wave_z_own.start()
        if c < line_first:
            start_z(c)

    wave_z_own.wait()
    wave_z_all.wait_recv()
    each_place(lambda py, px: wave_p(py, px, place).start())
    wave_p_own.start()
    for c in range(line_first, chunks):
        start_p(c)
    even[...] = jnp.zeros(even.shape, jnp.float32)
    odd[...] = jnp.zeros(odd.shape, jnp.float32)

    def drain_z(c):
        for g in groups_of(c):
            z_all(c, g).wait_send()

    def drain_p(c):
        p_all(c).wait_send()

    wait_z(0)
    start_p(0)
    wave_p_own.wait()
    wave_p_all.wait_recv()
    flat_waves = wave_all.reshape(OWNERS * 8, LANES)
    gathered = flat_waves[pl.ds(0, OWNERS, stride=8), :].astype(jnp.float32)
    for slot in range(slots):
        wave_rows[slot * OWNERS:(slot + 1) * OWNERS, :] = jnp.broadcast_to(
            gathered[:, slot:slot + 1], (OWNERS, LANES)
        )
    position = lax.broadcasted_iota(jnp.int32, (1, LANES), 1).astype(jnp.float32)
    sin_tiles = sin_hi.shape[1] // LANES

    def fill(i, carry):
        at = pl.ds(pl.multiple_of(i * 16, 16), 16)
        waves = wave_rows[at, :]
        weight = jnp.where(waves == 0.0, 1.0, 2.0)
        c, s = cos_sin(waves * position)
        turn_c, turn_s = cos_sin(waves * float(LANES))
        c, s = c * weight, s * weight
        for tile in range(sin_tiles + 1):
            to = slice(tile * LANES, (tile + 1) * LANES)
            top = c.astype(jnp.bfloat16)
            cos_hi[at, to] = top
            cos_lo[at, to] = (c - top.astype(jnp.float32)).astype(jnp.bfloat16)
            if tile < sin_tiles:
                top = s.astype(jnp.bfloat16)
                sin_hi[at, to] = top
                sin_lo[at, to] = (s - top.astype(jnp.float32)).astype(jnp.bfloat16)
                c, s = c * turn_c - s * turn_s, s * turn_c + c * turn_s
        return carry

    south = me // (OWNERS // 2)
    flat = recv.reshape(chunks * OWNERS * 8, LANES)

    def add_chunk(c, low_row=0, high_row=rows):
        parts = [[], []]
        for row in range(low_row, high_row):
            turned = flat[pl.ds(c * OWNERS * 8 + row, OWNERS, stride=8), :].T
            for part in range(2):
                parts[part].append(
                    jnp.concatenate(
                        [turned[part * levels:(part + 1) * levels],
                         turned[(2 + part) * levels:(3 + part) * levels]], 1
                    )
                )
        at = pl.ds(pl.multiple_of(c * 2 * OWNERS, 2 * OWNERS), 2 * OWNERS)
        for part, total, high, low in ((0, even, cos_hi, cos_lo), (1, odd, sin_hi, sin_lo)):
            values = jnp.concatenate(parts[part], 0)
            top = values.astype(jnp.bfloat16)
            rest = (values - top.astype(jnp.float32)).astype(jnp.bfloat16)
            table = high[at, :]
            sums = jnp.dot(top, table, preferred_element_type=jnp.float32)
            sums += jnp.dot(rest, table, preferred_element_type=jnp.float32)
            sums += jnp.dot(top, low[at, :], preferred_element_type=jnp.float32)
            total[low_row * levels:high_row * levels, :] += sums

    lax.fori_loop(0, wave_rows.shape[0] // 16, fill, 0)
    for c in range(1, line_first):
        if c == line_first - 1:
            wave_z_all.wait_send()
            wave_p_all.wait_send()
            drain_z(0)
            drain_p(line_first)
            drain_p(line_first + 1)
        wait_z(c)
        start_p(c)
        if line_first - 1 + c < chunks:
            wait_p(line_first - 1 + c)
            start_z(line_first - 1 + c)
        wait_p(c - 1)
        add_chunk(c - 1)
    wait_p(line_first - 1)
    add_chunk(line_first - 1)
    for c in range(line_first, chunks - 1):
        wait_z(c)
        add_chunk(c)

    r = lax.broadcasted_iota(jnp.int32, (TILE, TILE), 0)
    q = lax.broadcasted_iota(jnp.int32, (TILE, TILE), 1)
    mirror = jnp.where(r + q == TILE, 1.0, 0.0).astype(jnp.bfloat16)
    at_zero = lax.broadcasted_iota(jnp.int32, (1, TILE), 1) == 0
    tiles = odd.shape[1] // TILE

    def finish(low_row, high_row):
        at = slice(low_row * levels, high_row * levels)

        def put(values, to):
            for row in range(low_row, high_row):
                target = row + south * (rows - 1 - 2 * row)
                out[target, :, to] = values[(row - low_row) * levels:(row - low_row + 1) * levels]

        after = even[at, tiles * TILE:tiles * TILE + 1]
        for tile in range(tiles - 1, -1, -1):
            to = slice(tile * TILE, (tile + 1) * TILE)
            back = slice((2 * tiles - 1 - tile) * TILE, (2 * tiles - tile) * TILE)
            e, o = even[at, to], odd[at, to]
            put(e - o, to)
            d = e + o
            top = d.astype(jnp.bfloat16)
            rest = (d - top.astype(jnp.float32)).astype(jnp.bfloat16)
            turned = jnp.dot(top, mirror, preferred_element_type=jnp.float32)
            turned += jnp.dot(rest, mirror, preferred_element_type=jnp.float32)
            put(jnp.where(at_zero, after, turned), back)
            after = d[:, 0:1]

    for c in range(1, chunks - 1):
        drain_z(c)
    for c in range(line_first):
        drain_p(c)
    for g in range(groups):
        wait_z(chunks - 1, g)
        low_row, high_row = g * rows // groups, (g + 1) * rows // groups
        add_chunk(chunks - 1, low_row, high_row)
        finish(low_row, high_row)

    drain_z(chunks - 1)


def on_device(spectral, legendre, wavenumber):
    slots, degrees, _, levels = spectral.shape
    north = legendre.shape[2]
    rows = 2 * north // OWNERS
    chunks = slots // 2
    line_first = 3
    groups = 2
    coeff = jnp.transpose(spectral, (0, 2, 3, 1)).reshape(slots, 2 * levels, degrees)
    depth = slots * OWNERS
    half = NLON // 2
    f32, bf16, i32 = jnp.float32, jnp.bfloat16, jnp.int32
    grid = pl.pallas_call(
        functools.partial(transform_kernel, chunks, line_first, groups, rows),
        out_shape=pltpu.VMEM((rows, levels, NLON), f32),
        in_specs=[
            pl.BlockSpec(memory_space=pltpu.HBM),
            pl.BlockSpec(memory_space=pltpu.HBM),
            pl.BlockSpec(memory_space=pltpu.HBM),
        ],
        out_specs=pl.BlockSpec(memory_space=pltpu.VMEM),
        scratch_shapes=[
            pltpu.SMEM((slots,), i32),
            pltpu.VMEM((slots, 2 * levels, degrees), bf16),
            pltpu.VMEM((slots, degrees, north), bf16),
            pltpu.VMEM((2, north + 8, LANES), f32),
            pltpu.VMEM((chunks, NY, NZ, NX, 8, LANES), f32),
            pltpu.VMEM((line_first, NZ, NY, NX, 8, LANES), f32),
            pltpu.VMEM((chunks - line_first, PLANE, NZ, 8, LANES), f32),
            pltpu.VMEM((chunks, PLANE, NZ, 8, LANES), f32),
            pltpu.VMEM((8, LANES), i32),
            pltpu.VMEM((NZ, 8, LANES), i32),
            pltpu.VMEM((PLANE, NZ, 8, LANES), i32),
            pltpu.VMEM((depth, LANES), f32),
            pltpu.VMEM((depth, half + LANES), bf16),
            pltpu.VMEM((depth, half + LANES), bf16),
            pltpu.VMEM((depth, half), bf16),
            pltpu.VMEM((depth, half), bf16),
            pltpu.VMEM((rows * levels, half + LANES), f32),
            pltpu.VMEM((rows * levels, half), f32),
            pltpu.SemaphoreType.DMA((2, chunks)),
            pltpu.SemaphoreType.DMA((chunks + groups,)),
            pltpu.SemaphoreType.DMA((chunks + groups,)),
            pltpu.SemaphoreType.DMA((chunks + 1,)),
            pltpu.SemaphoreType.DMA((chunks + 1,)),
            pltpu.SemaphoreType.DMA((2, chunks + groups)),
            pltpu.SemaphoreType.DMA,
        ],
        compiler_params=pltpu.CompilerParams(
            collective_id=0, has_side_effects=True, vmem_limit_bytes=56 * 2**20,
        ),
    )(wavenumber, coeff, legendre)
    return jnp.transpose(grid, (0, 2, 1))


def solution(mesh):
    return jax.shard_map(
        on_device,
        mesh=mesh,
        in_specs=(P("wa", None, None, "lev"), P("wa", None, None), P("wa")),
        out_specs=P("wa", None, "lev"),
        check_vma=False,
    )
```

```python
import functools
import math

import jax
import jax.numpy as jnp
from jax import lax
from jax.experimental import pallas as pl
from jax.experimental.pallas import tpu as pltpu
from jax.sharding import PartitionSpec as P

NLON = 2560
TILE = 256
LANES = 128
NY, NZ, NX = 4, 8, 4
PLANE = NY * NX
OWNERS = NY * NZ * NX


def cos_sin(turns):
    quarter = jnp.floor(turns * (4.0 / NLON) + 0.5)
    x = (turns - quarter * (NLON // 4)) * (2.0 * math.pi / NLON)
    y = x * x
    s = x * (1.0 + y * (-1 / 6 + y * (1 / 120 + y * (-1 / 5040 + y * (1 / 362880)))))
    c = 1.0 + y * (-1 / 2 + y * (1 / 24 + y * (-1 / 720 + y * (1 / 40320 - y * (1 / 3628800)))))
    which = quarter.astype(jnp.int32) & 3
    odd = (which & 1) == 1
    cos_out = jnp.where(odd, s, c)
    sin_out = jnp.where(odd, c, s)
    cos_out = jnp.where((which == 1) | (which == 2), -cos_out, cos_out)
    sin_out = jnp.where(which >= 2, -sin_out, sin_out)
    return cos_out, sin_out


def transform_kernel(
    chunks, line_first, groups, rows,
    wave_hbm, spectral_hbm, legendre_hbm,
    out,
    wave_smem, spectral, legendre, staged, send, middle, spread, recv,
    wave_row, wave_mid, wave_all, wave_rows,
    cos_hi, cos_lo, sin_hi, sin_lo, even, odd,
    load_sem, z_send, z_recv, p_send, p_recv, own_sem, wave_sem,
):
    me = lax.axis_index("wa")
    y, z, x = me // (NZ * NX), (me // NX) % NZ, me % NX
    place = y * NX + x
    slots, columns, degrees = spectral.shape
    north = legendre.shape[2]
    levels = columns // 2

    def peer_at(py, pz, px):
        return (py * NZ + pz) * NX + px

    def remote(src, dst, send_sem, recv_sem, peer):
        return pltpu.make_async_remote_copy(
            src_ref=src, dst_ref=dst, send_sem=send_sem, recv_sem=recv_sem,
            device_id={"wa": peer}, device_id_type=pl.DeviceIdType.MESH,
        )

    def each_z(act):
        for d in (4, 3, 5, 2, 6, 1, 7):
            act((z + d) % NZ)

    def each_place(act):
        for d in (5, 15, 7, 13, 10, 6, 9, 14, 11, 2, 8, 1, 4, 3, 12):
            act((y + d // NX) % NY, (x + d % NX) % NX)

    def z_views(c, g, to, owner):
        if c < line_first:
            return send.at[c, :, to, :, 0:rows, :], middle.at[c, owner, :, :, 0:rows, :]
        part = slice(g * rows // groups, (g + 1) * rows // groups) if c == chunks - 1 else slice(0, rows)
        return spread.at[c - line_first, :, to, part, :], recv.at[c, :, owner, part, :]

    def z_copy(c, g, to, owner):
        src, dst = z_views(c, g, to, owner)
        return remote(src, dst, z_send.at[c + g], z_recv.at[c + g], peer_at(y, to, x))

    def z_own(c, g):
        src, dst = z_views(c, g, z, z)
        return pltpu.make_async_copy(src, dst, z_recv.at[c + g])

    def z_all(c, g, owners):
        if c < line_first:
            landed = middle.at[c, 0:owners, :, :, 0:rows, :]
        else:
            part = slice(g * rows // groups, (g + 1) * rows // groups) if c == chunks - 1 else slice(0, rows)
            landed = recv.at[c, :, 0:owners, part, :]
        return remote(landed, landed, z_send.at[c + g], z_recv.at[c + g], peer_at(y, (z + 1) % NZ, x))

    def p_all(c, owners):
        if c < line_first:
            landed = recv.at[c, 0:owners, :, 0:rows, :]
        else:
            landed = spread.at[c - line_first, 0:owners, :, 0:rows, :]
        return remote(landed, landed, p_send.at[c], p_recv.at[c], peer_at(y, z, (x + 1) % NX))

    def groups_of(c):
        return range(groups if c == chunks - 1 else 1)

    def p_copy(c, py, px, owner):
        if c < line_first:
            src, dst = middle.at[c, :, py, px, 0:rows, :], recv.at[c, owner, :, 0:rows, :]
        else:
            src = send.at[c, py, :, px, 0:rows, :]
            dst = spread.at[c - line_first, owner, :, 0:rows, :]
        return remote(
            src, dst, p_send.at[c], p_recv.at[c], peer_at(py, z, px)
        )

    def p_own(c):
        if c < line_first:
            src, dst = middle.at[c, :, y, x, 0:rows, :], recv.at[c, place, :, 0:rows, :]
        else:
            src = send.at[c, y, :, x, 0:rows, :]
            dst = spread.at[c - line_first, place, :, 0:rows, :]
        return pltpu.make_async_copy(src, dst, p_recv.at[c])

    def start_z(c):
        for g in groups_of(c):
            each_z(lambda to: z_copy(c, g, to, z).start())
            z_own(c, g).start()

    def start_p(c):
        each_place(lambda py, px: p_copy(c, py, px, place).start())
        p_own(c).start()

    def wait_z(c, g=0):
        z_all(c, g, NZ).wait_recv()

    def wait_p(c):
        p_all(c, PLANE).wait_recv()

    wave_job = chunks - 1 + groups

    def wave_z(to, owner):
        return remote(
            wave_row.at[0:1, :], wave_mid.at[owner, 0:1, :],
            z_send.at[wave_job], z_recv.at[wave_job], peer_at(y, to, x),
        )

    wave_z_own = pltpu.make_async_copy(
        wave_row.at[0:1, :], wave_mid.at[z, 0:1, :], own_sem.at[0]
    )

    def wave_p(py, px, owner):
        return remote(
            wave_mid.at[:, 0:1, :], wave_all.at[owner, :, 0:1, :],
            p_send.at[chunks], p_recv.at[chunks], peer_at(py, z, px),
        )

    wave_z_all = remote(
        wave_mid.at[0:NZ - 1, 0:1, :], wave_mid.at[0:NZ - 1, 0:1, :],
        z_send.at[wave_job], z_recv.at[wave_job], peer_at(y, (z + 1) % NZ, x),
    )
    wave_p_all = remote(
        wave_all.at[0:PLANE - 1, :, 0:1, :], wave_all.at[0:PLANE - 1, :, 0:1, :],
        p_send.at[chunks], p_recv.at[chunks], peer_at(y, z, (x + 1) % NX),
    )
    wave_p_own = pltpu.make_async_copy(
        wave_mid.at[:, 0:1, :], wave_all.at[place, :, 0:1, :], own_sem.at[1]
    )

    def load(c):
        pair = slice(2 * c, 2 * c + 2)
        return (
            pltpu.make_async_copy(legendre_hbm.at[pair], legendre.at[pair], load_sem.at[1, c]),
            pltpu.make_async_copy(spectral_hbm.at[pair], spectral.at[pair], load_sem.at[0, c]),
        )

    def start_load(c):
        for copy in load(c):
            copy.start()

    first_order = (0, 3, 1, 4, 2)
    own_waves = pltpu.make_async_copy(wave_hbm, wave_smem, wave_sem)
    own_waves.start()
    start_load(first_order[0])

    barrier = pltpu.get_barrier_semaphore()

    def greet(peer):
        pl.semaphore_signal(
            barrier, inc=1, device_id={"wa": peer}, device_id_type=pl.DeviceIdType.MESH
        )

    each_z(lambda to: greet(peer_at(y, to, x)))
    each_place(lambda py, px: greet(peer_at(py, z, px)))
    own_waves.wait()
    at_slot = lax.broadcasted_iota(jnp.int32, wave_row.shape, 1)
    waves = jnp.zeros(wave_row.shape, jnp.int32)
    for slot in range(slots):
        waves = jnp.where(at_slot == slot, wave_smem[slot], waves)
    wave_row[...] = waves
    staged[...] = jnp.zeros(staged.shape, jnp.float32)

    index = lax.broadcasted_iota(jnp.int32, (1, degrees), 1)

    def sums_of(slot):
        offset = index - wave_smem[slot]
        keep = jnp.where(offset >= 0, 1.0, 0.0)
        flip = jnp.where((offset & 1) == 0, keep, -keep)
        coeff = spectral[slot]
        both = jnp.concatenate(
            [coeff * keep.astype(coeff.dtype), coeff * flip.astype(coeff.dtype)], 0
        )
        return jnp.dot(both, legendre[slot], preferred_element_type=jnp.float32)

    def synthesize(c):
        first = sums_of(2 * c)
        second = sums_of(2 * c + 1)
        for side in range(2):
            part = slice(side * columns, (side + 1) * columns)
            staged[side, 0:north, :] = jnp.concatenate([first[part], second[part]], 0).T
            for slab in range(OWNERS // 2):
                d = OWNERS - 1 - slab if side else slab
                send[c, d // (NZ * NX), (d // NX) % NZ, d % NX] = staged[
                    side, rows * slab:rows * slab + 8, :
                ]

    for c in first_order:
        for copy in load(c):
            copy.wait()
        if c == first_order[0]:
            for other in first_order[1:]:
                start_load(other)
        synthesize(c)
        if c == first_order[0]:
            pl.semaphore_wait(barrier, NZ - 1 + PLANE - 1)
            each_z(lambda to: wave_z(to, z).start())
            wave_z_own.start()
        if c < line_first:
            start_z(c)

    wave_z_own.wait()
    wave_z_all.wait_recv()
    each_place(lambda py, px: wave_p(py, px, place).start())
    wave_p_own.start()
    for c in range(line_first, chunks):
        start_p(c)

    def drain_z(c):
        for g in groups_of(c):
            z_all(c, g, NZ - 1).wait_send()

    def drain_p(c):
        p_all(c, PLANE - 1).wait_send()

    wait_z(0)
    start_p(0)
    wave_p_own.wait()
    wave_p_all.wait_recv()
    flat_waves = wave_all.reshape(OWNERS * 8, LANES)
    gathered = flat_waves[pl.ds(0, OWNERS, stride=8), :].astype(jnp.float32)
    for slot in range(slots):
        wave_rows[slot * OWNERS:(slot + 1) * OWNERS, :] = jnp.broadcast_to(
            gathered[:, slot:slot + 1], (OWNERS, LANES)
        )
    position = lax.broadcasted_iota(jnp.int32, (1, LANES), 1).astype(jnp.float32)
    sin_tiles = sin_hi.shape[1] // LANES

    def fill(i, carry):
        at = pl.ds(pl.multiple_of(i * 16, 16), 16)
        waves = wave_rows[at, :]
        weight = jnp.where(waves == 0.0, 1.0, 2.0)
        c, s = cos_sin(waves * position)
        turn_c, turn_s = cos_sin(waves * float(LANES))
        c, s = c * weight, s * weight
        for tile in range(sin_tiles + 1):
            to = slice(tile * LANES, (tile + 1) * LANES)
            top = c.astype(jnp.bfloat16)
            cos_hi[at, to] = top
            cos_lo[at, to] = (c - top.astype(jnp.float32)).astype(jnp.bfloat16)
            if tile < sin_tiles:
                top = s.astype(jnp.bfloat16)
                sin_hi[at, to] = top
                sin_lo[at, to] = (s - top.astype(jnp.float32)).astype(jnp.bfloat16)
                c, s = c * turn_c - s * turn_s, s * turn_c + c * turn_s
        return carry

    south = me // (OWNERS // 2)
    flat = recv.reshape(chunks * OWNERS * 8, LANES)

    def add_chunk(c, low_row=0, high_row=rows):
        parts = [[], []]
        for row in range(low_row, high_row):
            turned = flat[pl.ds(c * OWNERS * 8 + row, OWNERS, stride=8), :].T
            for part in range(2):
                parts[part].append(
                    jnp.concatenate(
                        [turned[part * levels:(part + 1) * levels],
                         turned[(2 + part) * levels:(3 + part) * levels]], 1
                    )
                )
        at = pl.ds(pl.multiple_of(c * 2 * OWNERS, 2 * OWNERS), 2 * OWNERS)
        for part, total, high, low in ((0, even, cos_hi, cos_lo), (1, odd, sin_hi, sin_lo)):
            values = jnp.concatenate(parts[part], 0)
            top = values.astype(jnp.bfloat16)
            rest = (values - top.astype(jnp.float32)).astype(jnp.bfloat16)
            table = high[at, :]
            sums = jnp.dot(top, table, preferred_element_type=jnp.float32)
            sums += jnp.dot(rest, table, preferred_element_type=jnp.float32)
            sums += jnp.dot(top, low[at, :], preferred_element_type=jnp.float32)
            if c == 0:
                total[...] = sums
            else:
                total[low_row * levels:high_row * levels, :] += sums

    lax.fori_loop(0, wave_rows.shape[0] // 16, fill, 0)
    for c in range(1, line_first):
        if c == line_first - 1:
            wave_z_all.wait_send()
            wave_p_all.wait_send()
            drain_z(0)
            drain_p(line_first)
            drain_p(line_first + 1)
        wait_z(c)
        start_p(c)
        if line_first - 1 + c < chunks:
            wait_p(line_first - 1 + c)
            start_z(line_first - 1 + c)
        wait_p(c - 1)
        add_chunk(c - 1)
    wait_p(line_first - 1)
    add_chunk(line_first - 1)
    for c in range(line_first, chunks - 1):
        wait_z(c)
        add_chunk(c)

    r = lax.broadcasted_iota(jnp.int32, (TILE, TILE), 0)
    q = lax.broadcasted_iota(jnp.int32, (TILE, TILE), 1)
    mirror = jnp.where(r + q == TILE, 1.0, 0.0).astype(jnp.bfloat16)
    at_zero = lax.broadcasted_iota(jnp.int32, (1, TILE), 1) == 0
    tiles = odd.shape[1] // TILE

    def finish(low_row, high_row):
        at = slice(low_row * levels, high_row * levels)

        def put(values, to):
            for row in range(low_row, high_row):
                target = row + south * (rows - 1 - 2 * row)
                out[target, :, to] = values[(row - low_row) * levels:(row - low_row + 1) * levels]

        after = even[at, tiles * TILE:tiles * TILE + 1]
        for tile in range(tiles - 1, -1, -1):
            to = slice(tile * TILE, (tile + 1) * TILE)
            back = slice((2 * tiles - 1 - tile) * TILE, (2 * tiles - tile) * TILE)
            e, o = even[at, to], odd[at, to]
            put(e - o, to)
            d = e + o
            top = d.astype(jnp.bfloat16)
            rest = (d - top.astype(jnp.float32)).astype(jnp.bfloat16)
            turned = jnp.dot(top, mirror, preferred_element_type=jnp.float32)
            turned += jnp.dot(rest, mirror, preferred_element_type=jnp.float32)
            put(jnp.where(at_zero, after, turned), back)
            after = d[:, 0:1]

    for c in range(1, chunks - 1):
        drain_z(c)
    for c in range(line_first):
        drain_p(c)
    for g in range(groups):
        wait_z(chunks - 1, g)
        low_row, high_row = g * rows // groups, (g + 1) * rows // groups
        add_chunk(chunks - 1, low_row, high_row)
        finish(low_row, high_row)

    drain_z(chunks - 1)


def on_device(spectral, legendre, wavenumber):
    slots, degrees, _, levels = spectral.shape
    north = legendre.shape[2]
    rows = 2 * north // OWNERS
    chunks = slots // 2
    line_first = 3
    groups = 2
    coeff = jnp.transpose(spectral, (0, 2, 3, 1)).reshape(slots, 2 * levels, degrees)
    depth = slots * OWNERS
    half = NLON // 2
    f32, bf16, i32 = jnp.float32, jnp.bfloat16, jnp.int32
    grid = pl.pallas_call(
        functools.partial(transform_kernel, chunks, line_first, groups, rows),
        out_shape=pltpu.VMEM((rows, levels, NLON), f32),
        in_specs=[
            pl.BlockSpec(memory_space=pltpu.HBM),
            pl.BlockSpec(memory_space=pltpu.HBM),
            pl.BlockSpec(memory_space=pltpu.HBM),
        ],
        out_specs=pl.BlockSpec(memory_space=pltpu.VMEM),
        scratch_shapes=[
            pltpu.SMEM((slots,), i32),
            pltpu.VMEM((slots, 2 * levels, degrees), bf16),
            pltpu.VMEM((slots, degrees, north), bf16),
            pltpu.VMEM((2, north + 8, LANES), f32),
            pltpu.VMEM((chunks, NY, NZ, NX, 8, LANES), f32),
            pltpu.VMEM((line_first, NZ, NY, NX, 8, LANES), f32),
            pltpu.VMEM((chunks - line_first, PLANE, NZ, 8, LANES), f32),
            pltpu.VMEM((chunks, PLANE, NZ, 8, LANES), f32),
            pltpu.VMEM((8, LANES), i32),
            pltpu.VMEM((NZ, 8, LANES), i32),
            pltpu.VMEM((PLANE, NZ, 8, LANES), i32),
            pltpu.VMEM((depth, LANES), f32),
            pltpu.VMEM((depth, half + LANES), bf16),
            pltpu.VMEM((depth, half + LANES), bf16),
            pltpu.VMEM((depth, half), bf16),
            pltpu.VMEM((depth, half), bf16),
            pltpu.VMEM((rows * levels, half + LANES), f32),
            pltpu.VMEM((rows * levels, half), f32),
            pltpu.SemaphoreType.DMA((2, chunks)),
            pltpu.SemaphoreType.DMA((chunks + groups,)),
            pltpu.SemaphoreType.DMA((chunks + groups,)),
            pltpu.SemaphoreType.DMA((chunks + 1,)),
            pltpu.SemaphoreType.DMA((chunks + 1,)),
            pltpu.SemaphoreType.DMA((2,)),
            pltpu.SemaphoreType.DMA,
        ],
        compiler_params=pltpu.CompilerParams(
            collective_id=0, has_side_effects=True, vmem_limit_bytes=56 * 2**20,
        ),
    )(wavenumber, coeff, legendre)
    return jnp.transpose(grid, (0, 2, 1))


def solution(mesh):
    return jax.shard_map(
        on_device,
        mesh=mesh,
        in_specs=(P("wa", None, None, "lev"), P("wa", None, None), P("wa")),
        out_specs=P("wa", None, "lev"),
        check_vma=False,
    )
```

```python
import functools
import math

import jax
import jax.numpy as jnp
from jax import lax
from jax.experimental import pallas as pl
from jax.experimental.pallas import tpu as pltpu
from jax.sharding import PartitionSpec as P

NLON = 2560
TILE = 256
LANES = 128
NY, NZ, NX = 4, 8, 4
PLANE = NY * NX
OWNERS = NY * NZ * NX


def cos_sin(turns):
    quarter = jnp.floor(turns * (4.0 / NLON) + 0.5)
    x = (turns - quarter * (NLON // 4)) * (2.0 * math.pi / NLON)
    y = x * x
    s = x * (1.0 + y * (-1 / 6 + y * (1 / 120 + y * (-1 / 5040 + y * (1 / 362880)))))
    c = 1.0 + y * (-1 / 2 + y * (1 / 24 + y * (-1 / 720 + y * (1 / 40320 - y * (1 / 3628800)))))
    which = quarter.astype(jnp.int32) & 3
    odd = (which & 1) == 1
    cos_out = jnp.where(odd, s, c)
    sin_out = jnp.where(odd, c, s)
    cos_out = jnp.where((which == 1) | (which == 2), -cos_out, cos_out)
    sin_out = jnp.where(which >= 2, -sin_out, sin_out)
    return cos_out, sin_out


def transform_kernel(
    chunks, line_first, groups, rows,
    wave_hbm, spectral_hbm, legendre_hbm,
    out,
    wave_smem, spectral, legendre, staged, send, middle, spread, recv,
    wave_row, wave_mid, wave_all, wave_rows,
    cos_hi, cos_lo, sin_hi, sin_lo, even, odd,
    load_sem, z_send, z_recv, p_send, p_recv, own_sem, wave_sem,
):
    me = lax.axis_index("wa")
    y, z, x = me // (NZ * NX), (me // NX) % NZ, me % NX
    place = y * NX + x
    slots, columns, degrees = spectral.shape
    north = legendre.shape[2]
    levels = columns // 2

    def peer_at(py, pz, px):
        return (py * NZ + pz) * NX + px

    def remote(src, dst, send_sem, recv_sem, peer):
        return pltpu.make_async_remote_copy(
            src_ref=src, dst_ref=dst, send_sem=send_sem, recv_sem=recv_sem,
            device_id={"wa": peer}, device_id_type=pl.DeviceIdType.MESH,
        )

    def each_z(act):
        for d in (4, 3, 5, 2, 6, 1, 7):
            act((z + d) % NZ)

    def each_place(act):
        for d in (5, 15, 7, 13, 10, 6, 9, 14, 11, 2, 8, 1, 4, 3, 12):
            act((y + d // NX) % NY, (x + d % NX) % NX)

    def z_views(c, g, to, owner):
        if c < line_first:
            return send.at[c, :, to, :, 0:rows, :], middle.at[c, owner, :, :, 0:rows, :]
        part = slice(g * rows // groups, (g + 1) * rows // groups) if c == chunks - 1 else slice(0, rows)
        return spread.at[c - line_first, :, to, part, :], recv.at[c, :, owner, part, :]

    def z_copy(c, g, to, owner):
        src, dst = z_views(c, g, to, owner)
        return remote(src, dst, z_send.at[c + g], z_recv.at[c + g], peer_at(y, to, x))

    def z_own(c, g):
        src, dst = z_views(c, g, z, z)
        return pltpu.make_async_copy(src, dst, z_recv.at[c + g])

    def z_all(c, g, owners):
        if c < line_first:
            landed = middle.at[c, 0:owners, :, :, 0:rows, :]
        else:
            part = slice(g * rows // groups, (g + 1) * rows // groups) if c == chunks - 1 else slice(0, rows)
            landed = recv.at[c, :, 0:owners, part, :]
        return remote(landed, landed, z_send.at[c + g], z_recv.at[c + g], peer_at(y, (z + 1) % NZ, x))

    def p_all(c, owners):
        if c < line_first:
            landed = recv.at[c, 0:owners, :, 0:rows, :]
        else:
            landed = spread.at[c - line_first, 0:owners, :, 0:rows, :]
        return remote(landed, landed, p_send.at[c], p_recv.at[c], peer_at(y, z, (x + 1) % NX))

    def groups_of(c):
        return range(groups if c == chunks - 1 else 1)

    def p_copy(c, py, px, owner):
        if c < line_first:
            src, dst = middle.at[c, :, py, px, 0:rows, :], recv.at[c, owner, :, 0:rows, :]
        else:
            src = send.at[c, py, :, px, 0:rows, :]
            dst = spread.at[c - line_first, owner, :, 0:rows, :]
        return remote(
            src, dst, p_send.at[c], p_recv.at[c], peer_at(py, z, px)
        )

    def p_own(c):
        if c < line_first:
            src, dst = middle.at[c, :, y, x, 0:rows, :], recv.at[c, place, :, 0:rows, :]
        else:
            src = send.at[c, y, :, x, 0:rows, :]
            dst = spread.at[c - line_first, place, :, 0:rows, :]
        return pltpu.make_async_copy(src, dst, p_recv.at[c])

    def start_z(c):
        for g in groups_of(c):
            each_z(lambda to: z_copy(c, g, to, z).start())
            z_own(c, g).start()

    def start_p(c):
        each_place(lambda py, px: p_copy(c, py, px, place).start())
        p_own(c).start()

    def wait_z(c, g=0):
        z_all(c, g, NZ).wait_recv()

    def wait_p(c):
        p_all(c, PLANE).wait_recv()

    wave_job = chunks - 1 + groups

    def wave_z(to, owner):
        return remote(
            wave_row.at[0:1, :], wave_mid.at[owner, 0:1, :],
            z_send.at[wave_job], z_recv.at[wave_job], peer_at(y, to, x),
        )

    wave_z_own = pltpu.make_async_copy(
        wave_row.at[0:1, :], wave_mid.at[z, 0:1, :], own_sem.at[0]
    )

    def wave_p(py, px, owner):
        return remote(
            wave_mid.at[:, 0:1, :], wave_all.at[owner, :, 0:1, :],
            p_send.at[chunks], p_recv.at[chunks], peer_at(py, z, px),
        )

    wave_z_all = remote(
        wave_mid.at[0:NZ - 1, 0:1, :], wave_mid.at[0:NZ - 1, 0:1, :],
        z_send.at[wave_job], z_recv.at[wave_job], peer_at(y, (z + 1) % NZ, x),
    )
    wave_p_all = remote(
        wave_all.at[0:PLANE - 1, :, 0:1, :], wave_all.at[0:PLANE - 1, :, 0:1, :],
        p_send.at[chunks], p_recv.at[chunks], peer_at(y, z, (x + 1) % NX),
    )
    wave_p_own = pltpu.make_async_copy(
        wave_mid.at[:, 0:1, :], wave_all.at[place, :, 0:1, :], own_sem.at[1]
    )

    def load(c):
        pair = slice(2 * c, 2 * c + 2)
        return (
            pltpu.make_async_copy(legendre_hbm.at[pair], legendre.at[pair], load_sem.at[1, c]),
            pltpu.make_async_copy(spectral_hbm.at[pair], spectral.at[pair], load_sem.at[0, c]),
        )

    def start_load(c):
        for copy in load(c):
            copy.start()

    first_order = (0, 1, 2, 3, 4)
    own_waves = pltpu.make_async_copy(wave_hbm, wave_smem, wave_sem)
    own_waves.start()
    start_load(first_order[0])

    barrier = pltpu.get_barrier_semaphore()

    def greet(peer):
        pl.semaphore_signal(
            barrier, inc=1, device_id={"wa": peer}, device_id_type=pl.DeviceIdType.MESH
        )

    each_z(lambda to: greet(peer_at(y, to, x)))
    each_place(lambda py, px: greet(peer_at(py, z, px)))
    own_waves.wait()
    at_slot = lax.broadcasted_iota(jnp.int32, wave_row.shape, 1)
    waves = jnp.zeros(wave_row.shape, jnp.int32)
    for slot in range(slots):
        waves = jnp.where(at_slot == slot, wave_smem[slot], waves)
    wave_row[...] = waves
    staged[...] = jnp.zeros(staged.shape, jnp.float32)

    index = lax.broadcasted_iota(jnp.int32, (1, degrees), 1)

    def sums_of(slot):
        offset = index - wave_smem[slot]
        keep = jnp.where(offset >= 0, 1.0, 0.0)
        flip = jnp.where((offset & 1) == 0, keep, -keep)
        coeff = spectral[slot]
        both = jnp.concatenate(
            [coeff * keep.astype(coeff.dtype), coeff * flip.astype(coeff.dtype)], 0
        )
        return jnp.dot(both, legendre[slot], preferred_element_type=jnp.float32)

    def synthesize(c):
        first = sums_of(2 * c)
        second = sums_of(2 * c + 1)
        for side in range(2):
            part = slice(side * columns, (side + 1) * columns)
            staged[side, 0:north, :] = jnp.concatenate([first[part], second[part]], 0).T
            for slab in range(OWNERS // 2):
                d = OWNERS - 1 - slab if side else slab
                send[c, d // (NZ * NX), (d // NX) % NZ, d % NX] = staged[
                    side, rows * slab:rows * slab + 8, :
                ]

    for c in first_order:
        for copy in load(c):
            copy.wait()
        if c == first_order[0]:
            for other in first_order[1:]:
                start_load(other)
        synthesize(c)
        if c == first_order[0]:
            pl.semaphore_wait(barrier, NZ - 1 + PLANE - 1)
            each_z(lambda to: wave_z(to, z).start())
            wave_z_own.start()
        if c < line_first:
            start_z(c)

    wave_z_own.wait()
    wave_z_all.wait_recv()
    each_place(lambda py, px: wave_p(py, px, place).start())
    wave_p_own.start()
    for c in range(line_first, chunks):
        start_p(c)

    def drain_z(c):
        for g in groups_of(c):
            z_all(c, g, NZ - 1).wait_send()

    def drain_p(c):
        p_all(c, PLANE - 1).wait_send()

    wait_z(0)
    start_p(0)
    wave_p_own.wait()
    wave_p_all.wait_recv()
    flat_waves = wave_all.reshape(OWNERS * 8, LANES)
    gathered = flat_waves[pl.ds(0, OWNERS, stride=8), :].astype(jnp.float32)
    for slot in range(slots):
        wave_rows[slot * OWNERS:(slot + 1) * OWNERS, :] = jnp.broadcast_to(
            gathered[:, slot:slot + 1], (OWNERS, LANES)
        )
    position = lax.broadcasted_iota(jnp.int32, (1, LANES), 1).astype(jnp.float32)
    sin_tiles = sin_hi.shape[1] // LANES

    def fill(i, carry):
        at = pl.ds(pl.multiple_of(i * 16, 16), 16)
        waves = wave_rows[at, :]
        weight = jnp.where(waves == 0.0, 1.0, 2.0)
        c, s = cos_sin(waves * position)
        turn_c, turn_s = cos_sin(waves * float(LANES))
        c, s = c * weight, s * weight
        for tile in range(sin_tiles + 1):
            to = slice(tile * LANES, (tile + 1) * LANES)
            top = c.astype(jnp.bfloat16)
            cos_hi[at, to] = top
            cos_lo[at, to] = (c - top.astype(jnp.float32)).astype(jnp.bfloat16)
            if tile < sin_tiles:
                top = s.astype(jnp.bfloat16)
                sin_hi[at, to] = top
                sin_lo[at, to] = (s - top.astype(jnp.float32)).astype(jnp.bfloat16)
                c, s = c * turn_c - s * turn_s, s * turn_c + c * turn_s
        return carry

    south = me // (OWNERS // 2)
    flat = recv.reshape(chunks * OWNERS * 8, LANES)

    def add_chunk(c, low_row=0, high_row=rows):
        parts = [[], []]
        for row in range(low_row, high_row):
            turned = flat[pl.ds(c * OWNERS * 8 + row, OWNERS, stride=8), :].T
            for part in range(2):
                parts[part].append(
                    jnp.concatenate(
                        [turned[part * levels:(part + 1) * levels],
                         turned[(2 + part) * levels:(3 + part) * levels]], 1
                    )
                )
        at = pl.ds(pl.multiple_of(c * 2 * OWNERS, 2 * OWNERS), 2 * OWNERS)
        for part, total, high, low in ((0, even, cos_hi, cos_lo), (1, odd, sin_hi, sin_lo)):
            values = jnp.concatenate(parts[part], 0)
            top = values.astype(jnp.bfloat16)
            rest = (values - top.astype(jnp.float32)).astype(jnp.bfloat16)
            table = high[at, :]
            sums = jnp.dot(top, table, preferred_element_type=jnp.float32)
            sums += jnp.dot(rest, table, preferred_element_type=jnp.float32)
            sums += jnp.dot(top, low[at, :], preferred_element_type=jnp.float32)
            if c == 0:
                total[...] = sums
            else:
                total[low_row * levels:high_row * levels, :] += sums

    lax.fori_loop(0, wave_rows.shape[0] // 16, fill, 0)
    for c in range(1, line_first):
        if c == line_first - 1:
            wave_z_all.wait_send()
            wave_p_all.wait_send()
            drain_z(0)
            drain_p(line_first)
            drain_p(line_first + 1)
        wait_z(c)
        start_p(c)
        if line_first - 1 + c < chunks:
            wait_p(line_first - 1 + c)
            start_z(line_first - 1 + c)
        wait_p(c - 1)
        add_chunk(c - 1)
    wait_p(line_first - 1)
    add_chunk(line_first - 1)
    for c in range(line_first, chunks - 1):
        wait_z(c)
        add_chunk(c)

    r = lax.broadcasted_iota(jnp.int32, (TILE, TILE), 0)
    q = lax.broadcasted_iota(jnp.int32, (TILE, TILE), 1)
    mirror = jnp.where(r + q == TILE, 1.0, 0.0).astype(jnp.bfloat16)
    at_zero = lax.broadcasted_iota(jnp.int32, (1, TILE), 1) == 0
    tiles = odd.shape[1] // TILE

    def finish(low_row, high_row):
        at = slice(low_row * levels, high_row * levels)

        def put(values, to):
            for row in range(low_row, high_row):
                target = row + south * (rows - 1 - 2 * row)
                out[target, :, to] = values[(row - low_row) * levels:(row - low_row + 1) * levels]

        after = even[at, tiles * TILE:tiles * TILE + 1]
        for tile in range(tiles - 1, -1, -1):
            to = slice(tile * TILE, (tile + 1) * TILE)
            back = slice((2 * tiles - 1 - tile) * TILE, (2 * tiles - tile) * TILE)
            e, o = even[at, to], odd[at, to]
            put(e - o, to)
            d = e + o
            top = d.astype(jnp.bfloat16)
            rest = (d - top.astype(jnp.float32)).astype(jnp.bfloat16)
            turned = jnp.dot(top, mirror, preferred_element_type=jnp.float32)
            turned += jnp.dot(rest, mirror, preferred_element_type=jnp.float32)
            put(jnp.where(at_zero, after, turned), back)
            after = d[:, 0:1]

    for c in range(1, chunks - 1):
        drain_z(c)
    for c in range(line_first):
        drain_p(c)
    for g in range(groups):
        wait_z(chunks - 1, g)
        low_row, high_row = g * rows // groups, (g + 1) * rows // groups
        add_chunk(chunks - 1, low_row, high_row)
        finish(low_row, high_row)

    drain_z(chunks - 1)


def on_device(spectral, legendre, wavenumber):
    slots, degrees, _, levels = spectral.shape
    north = legendre.shape[2]
    rows = 2 * north // OWNERS
    chunks = slots // 2
    line_first = 3
    groups = 2
    coeff = jnp.transpose(spectral, (0, 2, 3, 1)).reshape(slots, 2 * levels, degrees)
    depth = slots * OWNERS
    half = NLON // 2
    f32, bf16, i32 = jnp.float32, jnp.bfloat16, jnp.int32
    grid = pl.pallas_call(
        functools.partial(transform_kernel, chunks, line_first, groups, rows),
        out_shape=pltpu.VMEM((rows, levels, NLON), f32),
        in_specs=[
            pl.BlockSpec(memory_space=pltpu.HBM),
            pl.BlockSpec(memory_space=pltpu.HBM),
            pl.BlockSpec(memory_space=pltpu.HBM),
        ],
        out_specs=pl.BlockSpec(memory_space=pltpu.VMEM),
        scratch_shapes=[
            pltpu.SMEM((slots,), i32),
            pltpu.VMEM((slots, 2 * levels, degrees), bf16),
            pltpu.VMEM((slots, degrees, north), bf16),
            pltpu.VMEM((2, north + 8, LANES), f32),
            pltpu.VMEM((chunks, NY, NZ, NX, 8, LANES), f32),
            pltpu.VMEM((line_first, NZ, NY, NX, 8, LANES), f32),
            pltpu.VMEM((chunks - line_first, PLANE, NZ, 8, LANES), f32),
            pltpu.VMEM((chunks, PLANE, NZ, 8, LANES), f32),
            pltpu.VMEM((8, LANES), i32),
            pltpu.VMEM((NZ, 8, LANES), i32),
            pltpu.VMEM((PLANE, NZ, 8, LANES), i32),
            pltpu.VMEM((depth, LANES), f32),
            pltpu.VMEM((depth, half + LANES), bf16),
            pltpu.VMEM((depth, half + LANES), bf16),
            pltpu.VMEM((depth, half), bf16),
            pltpu.VMEM((depth, half), bf16),
            pltpu.VMEM((rows * levels, half + LANES), f32),
            pltpu.VMEM((rows * levels, half), f32),
            pltpu.SemaphoreType.DMA((2, chunks)),
            pltpu.SemaphoreType.DMA((chunks + groups,)),
            pltpu.SemaphoreType.DMA((chunks + groups,)),
            pltpu.SemaphoreType.DMA((chunks + 1,)),
            pltpu.SemaphoreType.DMA((chunks + 1,)),
            pltpu.SemaphoreType.DMA((2,)),
            pltpu.SemaphoreType.DMA,
        ],
        compiler_params=pltpu.CompilerParams(
            collective_id=0, has_side_effects=True, vmem_limit_bytes=56 * 2**20,
        ),
    )(wavenumber, coeff, legendre)
    return jnp.transpose(grid, (0, 2, 1))


def solution(mesh):
    return jax.shard_map(
        on_device,
        mesh=mesh,
        in_specs=(P("wa", None, None, "lev"), P("wa", None, None), P("wa")),
        out_specs=P("wa", None, "lev"),
        check_vma=False,
    )
```
